32 devices in a mesh: ctx: 8 (over z, y), head: 4 (over x, core).
Axes of the slice: x: 2, y: 2, z: 4, core: 2. Of those that a mesh axis runs over, the one named last changes fastest.
Arguments:
- query_local: bfloat16 [1536, 5120], P(('ctx', 'head')), may hold values from -6 to 6
- key_local: bfloat16 [1536, 1024], P(('ctx', 'head')), may hold values from -6 to 6
- value_local: bfloat16 [1536, 1024], P(('ctx', 'head')), may hold values from -6 to 6
- stretch_labels: int32 [1536], replicated, may hold values from 0 to 3, never falling along the last dimension, each value on 1 to 768 neighbouring positions
- query_global: bfloat16 [1536, 5120], P(('ctx', 'head')), may hold values from -5 to 5
- key_global: bfloat16 [1536, 1024], P(('ctx', 'head')), may hold values from -5 to 5
- value_global: bfloat16 [1536, 1024], P(('ctx', 'head')), may hold values from -6 to 6
Outputs:
- local_heads: bfloat16 [1536, 5120], P(('ctx', 'head'))
- global_heads: bfloat16 [1536, 5120], P(('ctx', 'head'))
The draws below stay inside these ranges and needn't reach their ends.
Inputs may be any that keep to these rules, and one draw needn't show every extreme that they name: `stretch_labels`: stretches are runs of consecutive tokens; numbers never fall; each stretch has 1 to 768 tokens and some stretch has exactly 768.
All inputs are finite; a program needn't handle non-finite values.
Results may differ from the reference program's by a relative error of at most 0.0059.
Values may be sent and summed in bfloat16 or wider, within the bound.
No kernel may reach another device: no remote copies, remote signals or barrier semaphores. Data moves between devices by JAX's collectives and lax.ppermute only.
A program may use at most 128 MiB of HBM per device.

```python
import math
import jax
import jax.numpy as jnp
import numpy as np
from jax import lax

HEAD = 128
QH = 40
KVH = 8
TOK_DEV = 192
TOKENS = 1536
STRETCH = 768


def drawn(key):
    query_key = jax.random.fold_in(key, 11)
    key_stream = jax.random.fold_in(key, 12)
    query_width = QH * HEAD
    key_width = KVH * HEAD
    query_draw = jnp.clip(2.5 * jax.random.normal(query_key, (TOKENS, query_width), jnp.float32), -5.0, 5.0)
    key_draw = jnp.clip(jax.random.normal(key_stream, (TOKENS, key_width), jnp.float32), -4.0, 4.0)
    return (query_draw, key_draw)


def draw_query_global(key, part):
    return drawn(key)[0].astype(jnp.bfloat16)


def draw_key_global(key, part):
    return drawn(key)[1].astype(jnp.bfloat16)


def shard_levels(own_key, shape, pieces, smallest, largest):
    def one(position, parts):
        steps = jax.random.uniform(jax.random.fold_in(jax.random.fold_in(own_key, 6), position), (parts,), jnp.float32, smallest / len(pieces), largest / len(pieces))
        return jnp.repeat(jnp.exp(steps), shape[position] // parts).reshape((-1,) + (1,) * (len(shape) - position - 1))

    level = one(*pieces[0])
    for cut in pieces[1:]:
        level = level * one(*cut)
    return level


def profile(amount, total, limit, skew):
    weights = [(1 << 20) // math.isqrt(grade ** skew) + 1 for grade in range(2, amount + 1)]
    rest, counts = total - limit - (amount - 1), [1] * (amount - 1)
    while rest > 0:
        movable = [i for i in range(amount - 1) if counts[i] < limit]
        whole, budget = sum([weights[i] for i in movable]), rest
        for i in movable:
            addition = min(limit - counts[i], max(1, budget * weights[i] // whole), rest)
            counts[i] = counts[i] + addition
            rest = rest - addition
    return np.array([limit] + counts)


def uneven(rng, number_of, total, limit, slope):
    if number_of == 2:
        one = jax.random.randint(rng, (), max(1, total - limit), min(limit, total - 1) + 1)
        return jnp.stack([one, total - one])
    tallies = jnp.asarray(profile(number_of, total, limit, slope), jnp.int32)
    couples = (number_of - 1) // 2
    source_of, taker = tallies[1:1 + 2 * couples:2], tallies[2:2 + 2 * couples:2]
    margin = jnp.minimum(source_of - 1, limit - taker)
    moved = jax.random.randint(jax.random.fold_in(rng, 1), (couples,), 0, 1 << 20) % (margin + 1)
    tallies = tallies.at[1:1 + 2 * couples:2].set(source_of - moved).at[2:2 + 2 * couples:2].set(taker + moved)
    return tallies[jax.random.permutation(jax.random.fold_in(rng, 2), number_of)]


def bell_draw(stream_key, dims, scale, reach, shards=(), kind=jnp.bfloat16):
    drawn = jax.random.normal(stream_key, dims, jnp.float32) * scale
    if len(shards) > 0:
        drawn = shard_levels(stream_key, dims, shards, -0.22, 0.18) * drawn
    return jnp.clip(drawn, min=-reach, max=reach).astype(kind)


def setup_inputs(seed: int = 0) -> dict:
    arg_keys = jax.random.split(jax.random.key(seed), 8)
    query_local = bell_draw(arg_keys[0], (TOKENS, QH * HEAD), 1.0, 6.0, ((0, 32),))
    key_local = bell_draw(arg_keys[1], (TOKENS, KVH * HEAD), 1.0, 6.0, ((0, 32),))
    value_local = bell_draw(arg_keys[2], (TOKENS, KVH * HEAD), 1.0, 6.0, ((0, 32),))
    stretch_labels = jnp.searchsorted(jnp.cumsum(uneven(arg_keys[3], TOKENS // (2 * TOK_DEV), TOKENS, STRETCH, 2)), jnp.arange(TOKENS), side="right").astype(jnp.int32)
    query_global = draw_query_global(jax.random.fold_in(arg_keys[7], 71), 0)
    key_global = draw_key_global(jax.random.fold_in(arg_keys[7], 71), 0)
    value_global = bell_draw(arg_keys[6], (TOKENS, KVH * HEAD), 1.0, 6.0, ((0, 32),))
    return dict(query_local=query_local, key_local=key_local, value_local=value_local, stretch_labels=stretch_labels, query_global=query_global, key_global=key_global, value_global=value_global)


rope_base = 500000.0
norm_epsilon = 1e-06
temper_floor = 8192
temper_slope = 0.1
masked_score = -1e+30

def rotate(tensor, positions):
    head_width = tensor.shape[-1]
    half_width = head_width // 2
    frequency = rope_base ** (-(jnp.arange(half_width, dtype=jnp.float32) * 2.0 / head_width))
    angles = positions.astype(jnp.float32)[:, None] * frequency[None, :]
    extra_dims = tensor.ndim - 2
    angles = angles.reshape((angles.shape[0],) + (1,) * extra_dims + (half_width,))
    cosine = jnp.cos(angles)
    sine_part = jnp.sin(angles)
    first_part = tensor[..., :half_width]
    second_part = tensor[..., half_width:]
    return jnp.concatenate([first_part * cosine - second_part * sine_part, first_part * sine_part + second_part * cosine], axis=-1)

def normalize(tensor):
    return tensor * lax.rsqrt(lax.optimization_barrier(jnp.mean(tensor * tensor, axis=-1, keepdims=True)) + norm_epsilon)

def tempering(positions):
    return 1.0 + temper_slope * jnp.log(((positions + 1) // temper_floor + 1).astype(jnp.float32))

def reference(query_local, key_local, value_local, stretch_labels, query_global, key_global, value_global):
    length = query_local.shape[0]
    key_heads = key_local.shape[1] // HEAD
    group_size = query_local.shape[1] // (key_heads * HEAD)
    scaling = HEAD ** (-0.5)
    positions = jnp.arange(length, dtype=jnp.int32)
    query_shape = (length, key_heads, group_size, HEAD)
    key_shape = (length, key_heads, HEAD)
    queries = normalize(rotate(query_local.astype(jnp.float32).reshape(query_shape), positions)).astype(jnp.bfloat16)
    keys_normed = normalize(rotate(key_local.astype(jnp.float32).reshape(key_shape), positions)).astype(jnp.bfloat16)
    queries = lax.optimization_barrier(queries).astype(jnp.float32)
    keys_normed = lax.optimization_barrier(keys_normed).astype(jnp.float32)
    values_local = value_local.astype(jnp.float32).reshape(key_shape)
    block_rows = 256 if length % 256 == 0 else length
    reach_rows = STRETCH
    padded_keys = jnp.concatenate([jnp.zeros((reach_rows, key_heads, HEAD), jnp.float32), keys_normed], axis=0)
    padded_values = jnp.concatenate([jnp.zeros((reach_rows, key_heads, HEAD), jnp.float32), values_local], axis=0)
    padded_labels = jnp.concatenate([jnp.full((reach_rows,), -1, jnp.int32), stretch_labels.astype(jnp.int32)], axis=0)

    def local_block(anchor):
        query_block = lax.dynamic_slice_in_dim(queries, anchor, block_rows, 0)
        query_ids = lax.dynamic_slice_in_dim(stretch_labels.astype(jnp.int32), anchor, block_rows, 0)
        query_pos = anchor + jnp.arange(block_rows, dtype=jnp.int32)
        key_block = lax.dynamic_slice_in_dim(padded_keys, anchor, reach_rows + block_rows, 0)
        value_block = lax.dynamic_slice_in_dim(padded_values, anchor, reach_rows + block_rows, 0)
        key_ids = lax.dynamic_slice_in_dim(padded_labels, anchor, reach_rows + block_rows, 0)
        key_pos = anchor - reach_rows + jnp.arange(reach_rows + block_rows, dtype=jnp.int32)
        allowed = (key_ids[None, :] == query_ids[:, None]) & (key_pos[None, :] <= query_pos[:, None])
        scores = jnp.einsum('qhgd,khd->hgqk', query_block, key_block) * scaling
        weights = jnp.where(allowed[None, None], jnp.exp(scores), 0.0)
        totals = lax.optimization_barrier(jnp.sum(weights, axis=-1))
        rounded = lax.optimization_barrier(weights.astype(jnp.bfloat16)).astype(jnp.float32)
        weighted = jnp.einsum('hgqk,khd->qhgd', rounded, value_block)
        return (weighted / jnp.transpose(totals, (2, 0, 1))[..., None]).astype(jnp.bfloat16)
    anchors = jnp.arange(0, length, block_rows, dtype=jnp.int32)
    local_heads = lax.map(local_block, anchors).reshape(length, -1)
    query_rows = query_global.astype(jnp.float32).reshape(query_shape)
    key_rows = key_global.astype(jnp.float32).reshape(key_shape)
    value_rows = value_global.astype(jnp.float32).reshape(key_shape)
    temper_scale = tempering(positions) * scaling
    global_rows = 128 if length % 128 == 0 else length

    def global_block(anchor):
        query_block = lax.dynamic_slice_in_dim(query_rows, anchor, global_rows, 0)
        query_pos = anchor + jnp.arange(global_rows, dtype=jnp.int32)
        block_scale = lax.dynamic_slice_in_dim(temper_scale, anchor, global_rows, 0)
        scores = jnp.einsum('qhgd,khd->hgqk', query_block, key_rows) * block_scale[None, None, :, None]
        allowed = positions[None, :] <= query_pos[:, None]
        scores = jnp.where(allowed[None, None], scores, masked_score)
        row_peak = lax.optimization_barrier(jnp.max(scores, axis=-1))
        powers = jnp.where(allowed[None, None], jnp.exp(scores - row_peak[..., None]), 0.0)
        totals = lax.optimization_barrier(jnp.sum(powers, axis=-1))
        rounded = lax.optimization_barrier(powers.astype(jnp.bfloat16)).astype(jnp.float32)
        weighted = jnp.einsum('hgqk,khd->qhgd', rounded, value_rows)
        return (weighted / jnp.transpose(totals, (2, 0, 1))[..., None]).astype(jnp.bfloat16)
    global_anchors = jnp.arange(0, length, global_rows, dtype=jnp.int32)
    global_heads = lax.map(global_block, global_anchors).reshape(length, -1)
    return (local_heads, global_heads)
```

```python
import functools
import math

import jax
import jax.numpy as jnp
from jax import lax
from jax.experimental import pallas as pl
from jax.experimental.pallas import tpu as pltpu
from jax.sharding import Mesh
from jax.sharding import PartitionSpec as P

HEAD = 128
STRETCH = 768

rope_base = 500000.0
norm_epsilon = 1e-06
temper_floor = 8192
temper_slope = 0.1
masked_score = -1e30
log2e = 1.4426950408889634

IN_PLANE = ("row", "head")


def rope_tables(positions):
    half = HEAD // 2
    lane = lax.broadcasted_iota(jnp.int32, (1, HEAD), 1)
    index = jnp.where(lane < half, lane, lane - half).astype(jnp.float32)
    frequency = rope_base ** (-(index * 2.0 / HEAD))
    angles = positions.astype(jnp.float32)[:, None] * frequency
    sine = jnp.sin(angles)
    return jnp.cos(angles), jnp.where(lane < half, -sine, sine)


def rotated_unit(x, cosine, sine):
    y = x * cosine + pltpu.roll(x, HEAD // 2, 1) * sine
    return y * lax.rsqrt(jnp.mean(y * y, axis=-1, keepdims=True) + norm_epsilon)


def vmem_call(body, out_shapes, n_in, flops=0, nbytes=0, exps=0, scratch=(), smem=0):
    return pl.pallas_call(
        body,
        out_shape=out_shapes,
        in_specs=[pl.BlockSpec(memory_space=pltpu.SMEM)] * smem
        + [pl.BlockSpec(memory_space=pltpu.VMEM)] * n_in,
        out_specs=jax.tree.map(lambda _: pl.BlockSpec(memory_space=pltpu.VMEM), out_shapes),
        scratch_shapes=list(scratch),
        cost_estimate=pl.CostEstimate(flops=flops, bytes_accessed=nbytes, transcendentals=exps),
    )


def pack_pair_body(k_ref, v_ref, o_ref):
    for d in range(o_ref.shape[0]):
        o_ref[d, 0] = k_ref[:, d * HEAD : (d + 1) * HEAD]
        o_ref[d, 1] = v_ref[:, d * HEAD : (d + 1) * HEAD]


def pack_pair(key, value):
    tokens, width = key.shape
    shape = jax.ShapeDtypeStruct((width // HEAD, 2, tokens, HEAD), key.dtype)
    return vmem_call(pack_pair_body, shape, 2, nbytes=4 * key.size * 2)(key, value)


def pack_query_body(q_ref, cos_ref, sin_ref, o_ref):
    members = o_ref.shape[2] // HEAD
    cosine, sine = cos_ref[...], sin_ref[...]
    for d in range(o_ref.shape[0]):
        for g in range(members):
            at = (d * members + g) * HEAD
            x = q_ref[:, at : at + HEAD].astype(jnp.float32)
            o_ref[d, :, g * HEAD : (g + 1) * HEAD] = rotated_unit(x, cosine, sine).astype(o_ref.dtype)


def pack_plain_body(q_ref, o_ref):
    width = o_ref.shape[2]
    for d in range(o_ref.shape[0]):
        o_ref[d] = q_ref[:, d * width : (d + 1) * width]


def unpack_body(x_ref, o_ref):
    width = x_ref.shape[2]
    for d in range(x_ref.shape[0]):
        o_ref[:, d * width : (d + 1) * width] = x_ref[d]


def unpack(x):
    parts, tokens, width = x.shape
    shape = jax.ShapeDtypeStruct((tokens, parts * width), x.dtype)
    return vmem_call(unpack_body, shape, 1, nbytes=4 * x.size)(x)


def causal(rows):
    r = lax.broadcasted_iota(jnp.int32, (rows, rows), 0)
    c = lax.broadcasted_iota(jnp.int32, (rows, rows), 1)
    return c <= r


def extended(value):
    return jnp.concatenate([value, jnp.ones_like(value)], axis=1)


NT = (((1,), (1,)), ((), ()))


def local_body(n_back, plane_ref, *refs):
    q_ref, qid_ref, kid_ref, cos_ref, sin_ref = refs[:5]
    pairs = refs[5 : 5 + n_back + 1]
    o_ref, acc_ref, k_ref, v_ref = refs[5 + n_back + 1 :]
    parts, tokens, width = q_ref.shape
    rows = parts * tokens
    members = width // HEAD
    plane = plane_ref[0]
    scale = log2e * HEAD**-0.5
    q_all = q_ref.at[...]

    for d in range(n_back + 1):

        @pl.when(plane >= d)
        def _(d=d):
            keys = pairs[d][:, 0].reshape(rows, HEAD).astype(jnp.float32)
            k_ref[...] = rotated_unit(keys, cos_ref[d], sin_ref[d]).astype(k_ref.dtype)
            v_ref[...] = extended(pairs[d][:, 1].reshape(rows, HEAD))
            allowed = qid_ref[:, :1] == kid_ref[d, :1, :]
            if d == 0:
                allowed = allowed & causal(rows)

            def member(g, carry):
                at = pl.multiple_of(g * HEAD, HEAD)
                q = q_all[:, :, pl.ds(at, HEAD)].reshape(rows, HEAD)
                scores = lax.dot_general(q, k_ref[...], NT, preferred_element_type=jnp.float32)
                weights = jnp.where(allowed, jnp.exp2(scores * scale), 0.0).astype(jnp.bfloat16)
                part = jnp.dot(weights, v_ref[...], preferred_element_type=jnp.float32)
                if d == 0:
                    acc_ref[g] = part
                else:
                    acc_ref[g] += part
                return carry

            lax.fori_loop(0, members, member, 0)

    def finish(g, carry):
        at = pl.multiple_of(g * HEAD, HEAD)
        acc = acc_ref[g]
        out = (acc[:, :HEAD] / acc[:, HEAD:]).astype(o_ref.dtype)
        o_ref[:, :, pl.ds(at, HEAD)] = out.reshape(parts, tokens, HEAD)
        return carry

    lax.fori_loop(0, members, finish, 0)


def global_body(n_back, plane_ref, *refs):
    q_ref, scale_ref = refs[:2]
    pairs = refs[2 : 2 + n_back + 1]
    o_ref, acc_ref, peak_ref, v_ref = refs[2 + n_back + 1 :]
    parts, tokens, width = q_ref.shape
    rows = parts * tokens
    members = width // HEAD
    plane = plane_ref[0]

    for d in range(n_back + 1):

        @pl.when(plane >= d)
        def _(d=d):
            v_ref[...] = extended(pairs[d][:, 1].reshape(rows, HEAD))
            allowed = causal(rows) if d == 0 else None

            def member(g, carry):
                at = pl.multiple_of(g * HEAD, HEAD)
                q = q_ref[:, :, pl.ds(at, HEAD)].reshape(rows, HEAD)
                keys = pairs[d][:, 0].reshape(rows, HEAD)
                scores = lax.dot_general(q, keys, NT, preferred_element_type=jnp.float32)
                scores = scores * scale_ref[:, :1]
                if d == 0:
                    scores = jnp.where(allowed, scores, masked_score)
                    peak = jnp.max(scores, axis=1, keepdims=True)
                else:
                    before = peak_ref[g][:, :1]
                    peak = jnp.maximum(before, jnp.max(scores, axis=1, keepdims=True))
                weights = jnp.exp2(scores - peak).astype(jnp.bfloat16)
                part = jnp.dot(weights, v_ref[...], preferred_element_type=jnp.float32)
                peak_ref[g] = jnp.broadcast_to(peak, (rows, HEAD))
                if d == 0:
                    acc_ref[g] = part
                else:
                    acc_ref[g] = acc_ref[g] * jnp.exp2(before - peak) + part
                return carry

            lax.fori_loop(0, members, member, 0)

    def finish(g, carry):
        at = pl.multiple_of(g * HEAD, HEAD)
        acc = acc_ref[g]
        out = (acc[:, :HEAD] / acc[:, HEAD:]).astype(o_ref.dtype)
        o_ref[:, :, pl.ds(at, HEAD)] = out.reshape(parts, tokens, HEAD)
        return carry

    lax.fori_loop(0, members, finish, 0)


def exchange(x):
    return lax.all_to_all(x, IN_PLANE, split_axis=0, concat_axis=0, tiled=True)


def upward(x, by):
    size = lax.axis_size("plane")
    return lax.ppermute(x, "plane", [(i, i + by) for i in range(size - by)])


def gathered(own, n_back):
    blocks = [own]
    for d in range(1, n_back + 1):
        step = 1 if d < 3 else 3
        blocks.append(upward(blocks[d - step], step))
    return blocks


def shards(query_local, key_local, value_local, labels, query_global, key_global, value_global):
    planes = lax.axis_size("plane")
    plane = lax.axis_index("plane")
    parts = lax.axis_size("row") * lax.axis_size("head")
    spot = lax.axis_index("row") * lax.axis_size("head") + lax.axis_index("head")
    tokens = query_local.shape[0]
    width = query_local.shape[1] // parts
    members = width // HEAD
    rows = parts * tokens
    local_back = min(planes - 1, -(-(STRETCH - 1) // rows))

    local_pair = exchange(pack_pair(key_local, value_local))
    global_pair = exchange(pack_pair(key_global, value_global))
    local_blocks = gathered(local_pair, local_back)
    global_blocks = gathered(global_pair, planes - 1)

    own_pos = (plane * parts + spot) * tokens + jnp.arange(tokens, dtype=jnp.int32)
    cosine, sine = rope_tables(own_pos)
    packed = jax.ShapeDtypeStruct((parts, tokens, width), query_local.dtype)
    q_local = exchange(vmem_call(pack_query_body, packed, 3, nbytes=4 * query_local.size)(query_local, cosine, sine))
    q_global = exchange(vmem_call(pack_plain_body, packed, 1, nbytes=4 * query_local.size)(query_global))

    plane_arg = plane.reshape(1).astype(jnp.int32)
    row_pos = plane * rows + jnp.arange(rows, dtype=jnp.int32)
    back = jnp.arange(local_back + 1, dtype=jnp.int32)
    key_pos = ((plane - back)[:, None] * rows + jnp.arange(rows, dtype=jnp.int32)[None, :]).reshape(-1)
    k_cos, k_sin = rope_tables(key_pos)
    k_cos = k_cos.reshape(local_back + 1, rows, HEAD)
    k_sin = k_sin.reshape(local_back + 1, rows, HEAD)
    row_ids = lax.dynamic_slice_in_dim(labels, plane * rows, rows, 0)
    q_ids = jnp.broadcast_to(row_ids[:, None], (rows, HEAD))
    key_ids = jnp.stack(
        [lax.dynamic_slice_in_dim(labels, jnp.maximum(plane - d, 0) * rows, rows, 0) for d in range(local_back + 1)]
    )
    key_ids = jnp.broadcast_to(key_ids[:, None, :], (local_back + 1, 8, rows))
    temper = 1.0 + temper_slope * jnp.log(((row_pos + 1) // temper_floor + 1).astype(jnp.float32))
    scale = jnp.broadcast_to((temper * (log2e * HEAD**-0.5))[:, None], (rows, HEAD))

    out_shape = jax.ShapeDtypeStruct((parts, tokens, width), query_local.dtype)
    pair_flops = 2 * 3 * rows * rows * HEAD * members
    local_out = vmem_call(
        functools.partial(local_body, local_back),
        out_shape,
        5 + local_back + 1,
        flops=pair_flops * (local_back + 1),
        nbytes=4 * rows * width * 2,
        exps=rows * rows * members * (local_back + 1),
        scratch=[
            pltpu.VMEM((members, rows, 2 * HEAD), jnp.float32),
            pltpu.VMEM((rows, HEAD), jnp.bfloat16),
            pltpu.VMEM((rows, 2 * HEAD), jnp.bfloat16),
        ],
        smem=1,
    )(plane_arg, q_local, q_ids, key_ids, k_cos, k_sin, *local_blocks)
    local_heads = unpack(exchange(local_out))

    global_out = vmem_call(
        functools.partial(global_body, planes - 1),
        out_shape,
        2 + planes,
        flops=pair_flops * planes,
        nbytes=4 * rows * width * 2,
        exps=rows * rows * members * planes,
        scratch=[
            pltpu.VMEM((members, rows, 2 * HEAD), jnp.float32),
            pltpu.VMEM((members, rows, HEAD), jnp.float32),
            pltpu.VMEM((rows, 2 * HEAD), jnp.bfloat16),
        ],
        smem=1,
    )(plane_arg, q_global, scale, *global_blocks)
    global_heads = unpack(exchange(global_out))
    return local_heads, global_heads


def solution(mesh):
    ctx, head = mesh.shape["ctx"], mesh.shape["head"]

    def run(*args):
        key_heads = args[1].shape[1] // HEAD
        row = max(1, key_heads // head)
        grid = Mesh(mesh.devices.reshape(ctx // row, row, head), ("plane", "row", "head"))
        spread = P(("plane", "row", "head"), None)
        return jax.shard_map(
            shards,
            mesh=grid,
            in_specs=(spread, spread, spread, P(), spread, spread, spread),
            out_specs=(spread, spread),
            check_vma=False,
        )(*args)

    return run
```

```python
import functools

import jax
import jax.numpy as jnp
from jax import lax
from jax.experimental import pallas as pl
from jax.experimental.pallas import tpu as pltpu
from jax.sharding import Mesh
from jax.sharding import PartitionSpec as P


HEAD = 128
STRETCH = 768

rope_base = 500000.0
norm_epsilon = 1e-06
temper_floor = 8192
temper_slope = 0.1
masked_score = -1e30
log2e = 1.4426950408889634

IN_PLANE = ("row", "head")


def rope_tables(positions):
    half = HEAD // 2
    lane = lax.broadcasted_iota(jnp.int32, (1, HEAD), 1)
    index = jnp.where(lane < half, lane, lane - half).astype(jnp.float32)
    frequency = rope_base ** (-(index * 2.0 / HEAD))
    angles = positions.astype(jnp.float32)[:, None] * frequency
    sine = jnp.sin(angles)
    return jnp.cos(angles), jnp.where(lane < half, -sine, sine)


def rotated_unit(x, cosine, sine):
    y = x * cosine + pltpu.roll(x, HEAD // 2, 1) * sine
    return y * lax.rsqrt(jnp.mean(y * y, axis=-1, keepdims=True) + norm_epsilon)


def vmem_call(body, out_shapes, n_in, flops=0, nbytes=0, exps=0, scratch=(), smem=0):
    return pl.pallas_call(
        body,
        out_shape=out_shapes,
        in_specs=[pl.BlockSpec(memory_space=pltpu.SMEM)] * smem
        + [pl.BlockSpec(memory_space=pltpu.VMEM)] * n_in,
        out_specs=jax.tree.map(lambda _: pl.BlockSpec(memory_space=pltpu.VMEM), out_shapes),
        scratch_shapes=list(scratch),
        cost_estimate=pl.CostEstimate(flops=flops, bytes_accessed=nbytes, transcendentals=exps),
    )


def pack_body(kl_ref, vl_ref, kg_ref, vg_ref, o_ref):
    for d in range(o_ref.shape[0]):
        for a, ref in enumerate((kl_ref, vl_ref, kg_ref, vg_ref)):
            o_ref[d, a] = ref[:, d * HEAD : (d + 1) * HEAD]


def pack_query_body(ql_ref, qg_ref, cos_ref, sin_ref, turn_ref, temper_ref, o_ref):
    members = o_ref.shape[3] // HEAD
    cosine, sine = cos_ref[...], sin_ref[...]
    for d in range(o_ref.shape[0]):
        for g in range(members):
            at = (d * members + g) * HEAD
            x = ql_ref[:, at : at + HEAD]
            turned = jnp.dot(x, turn_ref[...], preferred_element_type=jnp.float32)
            y = x.astype(jnp.float32) * cosine + turned * sine
            y = y * lax.rsqrt(jnp.mean(y * y, axis=-1, keepdims=True) + norm_epsilon)
            to = slice(g * HEAD, (g + 1) * HEAD)
            o_ref[d, 0, :, to] = y.astype(o_ref.dtype)
            z = qg_ref[:, at : at + HEAD].astype(jnp.float32) * temper_ref[...]
            o_ref[d, 1, :, to] = z.astype(o_ref.dtype)


def causal(rows):
    r = lax.broadcasted_iota(jnp.int32, (rows, rows), 0)
    c = lax.broadcasted_iota(jnp.int32, (rows, rows), 1)
    return c <= r


NT = (((1,), (1,)), ((), ()))


def local_body(n_back, plane_ref, *refs):
    q_ref, qid_ref, kid_ref, cos_ref, sin_ref = refs[:5]
    blocks = refs[5 : 5 + n_back + 1]
    o_ref, k_ref, v_ref = refs[5 + n_back + 1 :]
    parts, _, tokens, width = q_ref.shape
    rows = parts * tokens
    members = width // HEAD
    scale = log2e * HEAD**-0.5
    for d in range(n_back + 1):
        keys = blocks[d][:, 0].reshape(rows, HEAD).astype(jnp.float32)
        k_ref[d] = rotated_unit(keys, cos_ref[d], sin_ref[d]).astype(k_ref.dtype)
        v_ref[d, :, :HEAD] = blocks[d][:, 1].reshape(rows, HEAD)
        v_ref[d, :, HEAD:] = jnp.ones((rows, HEAD), v_ref.dtype)
    qid = jnp.concatenate([qid_ref[...]] * (rows // HEAD), axis=1)

    def member(g, carry):
        at = pl.multiple_of(g * HEAD, HEAD)
        q = q_ref[:, 0, :, pl.ds(at, HEAD)].reshape(rows, HEAD)
        acc = None
        for d in range(n_back + 1):
            allowed = qid == kid_ref[d, :1, :]
            if d == 0:
                allowed = allowed & causal(rows)
            scores = lax.dot_general(q, k_ref[d], NT, preferred_element_type=jnp.float32)
            weights = jnp.where(allowed, jnp.exp2(scores * scale), 0.0).astype(jnp.bfloat16)
            part = jnp.dot(weights, v_ref[d], preferred_element_type=jnp.float32)
            acc = part if acc is None else acc + part
        out = (acc[:, :HEAD] / acc[:, HEAD:]).astype(o_ref.dtype)
        o_ref[:, :, pl.ds(at, HEAD)] = out.reshape(parts, tokens, HEAD)
        return carry

    lax.fori_loop(0, members, member, 0)


def global_body(distances, plane_ref, *refs):
    n = len(distances)
    q_ref = refs[0]
    blocks = refs[1 : 1 + n]
    o_ref, v_ref = refs[1 + n :]
    parts, _, tokens, width = q_ref.shape
    rows = parts * tokens
    members = width // HEAD
    plane = plane_ref[0]
    scale = log2e * HEAD**-0.5
    for i in range(n):
        v_ref[i, :, :HEAD] = blocks[i][:, blocks[i].shape[1] - 1].reshape(rows, HEAD)
        v_ref[i, :, HEAD:] = jnp.ones((rows, HEAD), v_ref.dtype)

    def member(g, carry):
        at = pl.multiple_of(g * HEAD, HEAD)
        q = q_ref[:, 1, :, pl.ds(at, HEAD)].reshape(rows, HEAD)
        peak, acc = None, None
        for first in range(0, n, 4):
            group = range(first, min(n, first + 4))
            every, new_peak = [], peak
            for i in group:
                keys = blocks[i][:, blocks[i].shape[1] - 2].reshape(rows, HEAD)
                scores = lax.dot_general(q, keys, NT, preferred_element_type=jnp.float32)
                if distances[i] == 0:
                    scores = jnp.where(causal(rows), scores, masked_score)
                every.append(scores)
                top = scores[:, :HEAD]
                for j in range(HEAD, rows, HEAD):
                    top = jnp.maximum(top, scores[:, j : j + HEAD])
                top = jnp.max(top, axis=1, keepdims=True) * scale
                if distances[i] > 0:
                    top = jnp.where(plane >= distances[i], top, masked_score)
                new_peak = top if new_peak is None else jnp.maximum(new_peak, top)
            if acc is not None:
                acc = acc * jnp.exp2(peak - new_peak)
            peak = new_peak
            for i, scores in zip(group, every):
                shift = peak
                if distances[i] > 0:
                    shift = jnp.where(plane >= distances[i], peak, -masked_score)
                weights = jnp.exp2(scores * scale - shift).astype(jnp.bfloat16)
                part = jnp.dot(weights, v_ref[i], preferred_element_type=jnp.float32)
                acc = part if acc is None else acc + part
        out = (acc[:, :HEAD] / acc[:, HEAD:]).astype(o_ref.dtype)
        o_ref[:, :, pl.ds(at, HEAD)] = out.reshape(parts, tokens, HEAD)
        return carry

    lax.fori_loop(0, members, member, 0)


def exchange(x):
    return lax.all_to_all(x, IN_PLANE, split_axis=0, concat_axis=0, tiled=True)


def upward(x, by):
    size = lax.axis_size("plane")
    return lax.ppermute(x, "plane", [(i, i + by) for i in range(size - by)])


def unpack(x):
    parts, tokens, width = x.shape
    return x.transpose(1, 0, 2).reshape(tokens, parts * width)


def shards(query_local, key_local, value_local, labels, query_global, key_global, value_global):
    planes = lax.axis_size("plane")
    plane = lax.axis_index("plane")
    parts = lax.axis_size("row") * lax.axis_size("head")
    spot = lax.axis_index("row") * lax.axis_size("head") + lax.axis_index("head")
    tokens = query_local.shape[0]
    width = query_local.shape[1] // parts
    members = width // HEAD
    rows = parts * tokens
    dtype = query_local.dtype
    local_back = min(planes - 1, -(-(STRETCH - 1) // rows))

    packed = jax.ShapeDtypeStruct((parts, 4, tokens, HEAD), dtype)
    pack = vmem_call(pack_body, packed, 4, nbytes=16 * key_local.size)
    pack = pack(key_local, value_local, key_global, value_global)
    own = exchange(pack)
    local_blocks, global_blocks = [own], [own]
    for d in range(1, planes):
        if d == 1:
            came = upward(own, 1)
            local_blocks.append(came)
            global_blocks.append(came)
        elif d == 2:
            if d <= local_back:
                local_blocks.append(upward(came[:, :2], 1))
            global_blocks.append(upward(came[:, 2:], 1))
        else:
            if d <= local_back:
                local_blocks.append(upward(local_blocks[d - 3][:, :2], 3))
            source = global_blocks[d - 3]
            global_blocks.append(upward(source[:, source.shape[1] - 2 :], 3))

    own_pos = (plane * parts + spot) * tokens + jnp.arange(tokens, dtype=jnp.int32)
    cosine, sine = rope_tables(own_pos)
    half = HEAD // 2
    i, j = lax.broadcasted_iota(jnp.int32, (HEAD, HEAD), 0), lax.broadcasted_iota(jnp.int32, (HEAD, HEAD), 1)
    turn = jnp.where((i + half) % HEAD == j, 1.0, 0.0).astype(dtype)
    temper = 1.0 + temper_slope * jnp.log(((own_pos + 1) // temper_floor + 1).astype(jnp.float32))
    temper = jnp.broadcast_to(temper[:, None], (tokens, HEAD))
    packed = jax.ShapeDtypeStruct((parts, 2, tokens, width), dtype)
    pack = vmem_call(pack_query_body, packed, 6, nbytes=8 * query_local.size, flops=2 * HEAD * query_local.size)
    pack = pack(query_local, query_global, cosine, sine, turn, temper)
    queries = exchange(pack)

    plane_arg = plane.reshape(1).astype(jnp.int32)
    back = jnp.arange(local_back + 1, dtype=jnp.int32)
    key_pos = ((plane - back)[:, None] * rows + jnp.arange(rows, dtype=jnp.int32)[None, :]).reshape(-1)
    k_cos, k_sin = rope_tables(key_pos)
    k_cos = k_cos.reshape(local_back + 1, rows, HEAD)
    k_sin = k_sin.reshape(local_back + 1, rows, HEAD)
    row_ids = lax.dynamic_slice_in_dim(labels, plane * rows, rows, 0)
    q_ids = jnp.broadcast_to(row_ids[:, None], (rows, HEAD))
    key_ids = []
    for d in range(local_back + 1):
        ids = lax.dynamic_slice_in_dim(labels, jnp.maximum(plane - d, 0) * rows, rows, 0)
        key_ids.append(jnp.where(plane >= d, ids, -1))
    key_ids = jnp.broadcast_to(jnp.stack(key_ids)[:, None, :], (local_back + 1, 8, rows))

    out_shape = jax.ShapeDtypeStruct((parts, tokens, width), dtype)
    pair_flops = 2 * 3 * rows * rows * HEAD * members
    local_out = vmem_call(
        functools.partial(local_body, local_back),
        out_shape,
        5 + local_back + 1,
        flops=pair_flops * (local_back + 1),
        nbytes=4 * rows * width * 2,
        exps=rows * rows * members * (local_back + 1),
        scratch=[
            pltpu.VMEM((local_back + 1, rows, HEAD), jnp.bfloat16),
            pltpu.VMEM((local_back + 1, rows, 2 * HEAD), jnp.bfloat16),
        ],
        smem=1,
    )(plane_arg, queries, q_ids, key_ids, k_cos, k_sin, *local_blocks)
    local_heads = exchange(local_out)
    global_out = vmem_call(
        functools.partial(global_body, tuple(range(planes))),
        out_shape,
        1 + planes,
        flops=pair_flops * planes,
        nbytes=4 * rows * width * 2,
        exps=rows * rows * members * planes,
        scratch=[pltpu.VMEM((planes, rows, 2 * HEAD), jnp.bfloat16)],
        smem=1,
    )(plane_arg, queries, *global_blocks)
    global_heads = exchange(global_out)
    return unpack(local_heads), unpack(global_heads)


def solution(mesh):
    ctx, head = mesh.shape["ctx"], mesh.shape["head"]

    def run(*args):
        key_heads = args[1].shape[1] // HEAD
        row = max(1, key_heads // head)
        grid = Mesh(mesh.devices.reshape(ctx // row, row, head), ("plane", "row", "head"))
        spread = P(("plane", "row", "head"), None)
        return jax.shard_map(
            shards,
            mesh=grid,
            in_specs=(spread, spread, spread, P(), spread, spread, spread),
            out_specs=(spread, spread),
            check_vma=False,
        )(*args)

    return run
```

```python
import functools

import jax
import jax.numpy as jnp
import numpy as np
from jax import lax
from jax.experimental import pallas as pl
from jax.experimental.pallas import tpu as pltpu
from jax.sharding import Mesh
from jax.sharding import PartitionSpec as P


HEAD = 128
STRETCH = 768

rope_base = 500000.0
norm_epsilon = 1e-06
temper_floor = 8192
temper_slope = 0.1
masked_score = -1e30
log2e = 1.4426950408889634
far = 30000.0

IN_PLANE = ("row", "head")


def rope_tables(count, step):
    half = HEAD // 2
    frequency = rope_base ** (-(np.arange(HEAD) % half) * 2.0 / HEAD)
    angles = (np.arange(count) * step)[:, None] * frequency[None, :]
    sign = np.where(np.arange(HEAD) < half, -1.0, 1.0)
    return jnp.asarray(np.cos(angles), jnp.float32), jnp.asarray(np.sin(angles) * sign, jnp.float32)


def turned(cos_base, sin_base, cos_row, sin_row):
    return cos_base * cos_row - sin_base * sin_row, sin_base * cos_row + cos_base * sin_row


def rotated_unit(x, turn, cosine, sine):
    swapped = jnp.dot(x, turn, preferred_element_type=jnp.float32)
    y = x.astype(jnp.float32) * cosine + swapped * sine
    return y * lax.rsqrt(jnp.mean(y * y, axis=-1, keepdims=True) + norm_epsilon)


def vmem_call(body, out_shapes, n_in, flops=0, nbytes=0, exps=0, scratch=(), smem=0):
    return pl.pallas_call(
        body,
        out_shape=out_shapes,
        in_specs=[pl.BlockSpec(memory_space=pltpu.SMEM)] * smem
        + [pl.BlockSpec(memory_space=pltpu.VMEM)] * n_in,
        out_specs=jax.tree.map(lambda _: pl.BlockSpec(memory_space=pltpu.VMEM), out_shapes),
        scratch_shapes=list(scratch),
        cost_estimate=pl.CostEstimate(flops=flops, bytes_accessed=nbytes, transcendentals=exps),
    )


def pack_body(kl_ref, vl_ref, kg_ref, vg_ref, o_ref):
    for d in range(o_ref.shape[0]):
        for a, ref in enumerate((kl_ref, vl_ref, kg_ref, vg_ref)):
            o_ref[d, a] = ref[:, d * HEAD : (d + 1) * HEAD]


def pack_query_body(where_ref, ql_ref, qg_ref, cosb_ref, sinb_ref, cosr_ref, sinr_ref, turn_ref, temper_ref, o_ref):
    members = o_ref.shape[3] // HEAD
    tokens = ql_ref.shape[0]
    plane, first = where_ref[0], pl.multiple_of(where_ref[1], 16)
    mine = pl.ds(first, tokens)
    cosine, sine = turned(cosb_ref[pl.ds(plane, 1)], sinb_ref[pl.ds(plane, 1)], cosr_ref[mine], sinr_ref[mine])
    turn = turn_ref[...]
    for d in range(o_ref.shape[0]):
        for g in range(members):
            at = (d * members + g) * HEAD
            to = slice(g * HEAD, (g + 1) * HEAD)
            y = rotated_unit(ql_ref[:, at : at + HEAD], turn, cosine, sine)
            o_ref[d, 0, :, to] = y.astype(o_ref.dtype)
            z = qg_ref[:, at : at + HEAD].astype(jnp.float32) * temper_ref[...]
            o_ref[d, 1, :, to] = z.astype(o_ref.dtype)


def causal(rows):
    r = lax.broadcasted_iota(jnp.int32, (rows, rows), 0)
    c = lax.broadcasted_iota(jnp.int32, (rows, rows), 1)
    return c <= r


NT = (((1,), (1,)), ((), ()))


def take_values(v_ref, i, values, valid):
    rows = values.shape[0]
    v_ref[i * rows : (i + 1) * rows, :HEAD] = values
    ones = jnp.broadcast_to(jnp.where(valid, 1.0, 0.0), (rows, HEAD))
    v_ref[i * rows : (i + 1) * rows, HEAD:] = ones.astype(v_ref.dtype)


def divided(acc, dtype):
    return (acc[:, :HEAD] / acc[:, HEAD:]).astype(dtype)


def local_body(n_back, where_ref, *refs):
    q_ref, labels_ref, cosb_ref, sinb_ref, cosr_ref, sinr_ref, turn_ref = refs[:7]
    blocks = refs[7 : 7 + n_back + 1]
    o_ref, k_ref, v_ref = refs[7 + n_back + 1 :]
    parts, _, tokens, width = q_ref.shape
    rows = parts * tokens
    members = width // HEAD
    plane = where_ref[0]
    scale = log2e * HEAD**-0.5
    turn = turn_ref[...]
    lane = lax.broadcasted_iota(jnp.int32, (HEAD, rows), 0)
    for d in range(n_back + 1):
        behind = jnp.maximum(plane - d, 0)
        base = pl.ds(behind, 1)
        cosine, sine = turned(cosb_ref[base], sinb_ref[base], cosr_ref[...], sinr_ref[...])
        at = slice(d * rows, (d + 1) * rows)
        keys = blocks[d][:, 0].reshape(rows, HEAD)
        k_ref[at, :HEAD] = rotated_unit(keys, turn, cosine, sine).astype(k_ref.dtype)
        ids = labels_ref[:, pl.ds(pl.multiple_of(behind * rows, HEAD), rows)]
        same = jnp.where(lane == ids, 1.0, 0.0).T
        k_ref[at, HEAD:] = same.astype(k_ref.dtype)
        if d == 0:
            other = ((same - 1.0) * far).astype(k_ref.dtype)
        take_values(v_ref, d, blocks[d][:, 1].reshape(rows, HEAD), plane >= d)

    def member(g, carry):
        at = pl.multiple_of(g * HEAD, HEAD)
        q = jnp.concatenate([q_ref[:, 0, :, pl.ds(at, HEAD)].reshape(rows, HEAD), other], axis=1)
        scores = lax.dot_general(q, k_ref[...], NT, preferred_element_type=jnp.float32)
        weights = jnp.exp2(scores * scale)
        first = jnp.where(causal(rows), weights[:, :rows], 0.0)
        weights = jnp.concatenate([first, weights[:, rows:]], axis=1).astype(jnp.bfloat16)
        acc = jnp.dot(weights, v_ref[...], preferred_element_type=jnp.float32)
        o_ref[:, :, pl.ds(at, HEAD)] = divided(acc, o_ref.dtype).reshape(parts, tokens, HEAD)
        return carry

    lax.fori_loop(0, members, member, 0, unroll=True)


def global_body(n, where_ref, *refs):
    q_ref = refs[0]
    blocks = refs[1 : 1 + n]
    o_ref, k_ref, v_ref = refs[1 + n :]
    parts, _, tokens, width = q_ref.shape
    rows = parts * tokens
    members = width // HEAD
    plane = where_ref[0]
    scale = log2e * HEAD**-0.5
    groups = [(i, min(n, i + 4)) for i in range(0, n, 4)]
    for i in range(n):
        last = blocks[i].shape[1] - 1
        k_ref[i * rows : (i + 1) * rows] = blocks[i][:, last - 1].reshape(rows, HEAD)
        take_values(v_ref, i, blocks[i][:, last].reshape(rows, HEAD), plane >= i)

    def query(g):
        at = pl.multiple_of(g * HEAD, HEAD)
        return q_ref[:, 1, :, pl.ds(at, HEAD)].reshape(rows, HEAD)

    def put(g, acc):
        at = pl.multiple_of(g * HEAD, HEAD)
        o_ref[:, :, pl.ds(at, HEAD)] = divided(acc, o_ref.dtype).reshape(parts, tokens, HEAD)

    def scored(q, group):
        keys = k_ref[group[0] * rows : group[1] * rows]
        return lax.dot_general(q, keys, NT, preferred_element_type=jnp.float32) * scale

    def summed(weights, group):
        if group[0] == 0:
            first = jnp.where(causal(rows), weights[:, :rows], 0.0)
            weights = jnp.concatenate([first, weights[:, rows:]], axis=1)
        values = v_ref[group[0] * rows : group[1] * rows]
        return jnp.dot(weights.astype(jnp.bfloat16), values, preferred_element_type=jnp.float32)

    def plain(g, carry):
        low, high = carry
        q = query(g)
        acc = summed(jnp.exp2(scored(q, groups[0])), groups[0])
        for group in groups[1:]:
            acc = acc + summed(jnp.exp2(scored(q, group)), group)
        put(g, acc)
        totals = acc[:, HEAD:]
        low = jnp.minimum(low, jnp.min(totals, axis=0, keepdims=True))
        high = jnp.maximum(high, jnp.max(totals, axis=0, keepdims=True))
        return low, high

    ones = jnp.ones((1, HEAD), jnp.float32)
    low, high = lax.fori_loop(0, members, plain, (ones, ones), unroll=len(groups) == 1)
    safe = (jnp.min(low) > 2.0**-80) & (jnp.max(high) < 2.0**100)

    @pl.when(jnp.logical_not(safe))
    def _():
        def shifted(g, carry):
            q = query(g)
            peak, acc = None, None
            for group in groups:
                scores = scored(q, group)
                parts_of = []
                for i in range(group[0], group[1]):
                    part = scores[:, (i - group[0]) * rows : (i - group[0] + 1) * rows]
                    if i == 0:
                        part = jnp.where(causal(rows), part, masked_score)
                    else:
                        part = jnp.where(plane >= i, part, masked_score)
                    parts_of.append(part)
                scores = jnp.concatenate(parts_of, axis=1)
                top = jnp.max(scores, axis=1, keepdims=True)
                new_peak = top if peak is None else jnp.maximum(peak, top)
                if acc is not None:
                    acc = acc * jnp.exp2(peak - new_peak)
                peak = new_peak
                part = summed(jnp.exp2(scores - peak), group)
                acc = part if acc is None else acc + part
            put(g, acc)
            return carry

        lax.fori_loop(0, members, shifted, 0)


def exchange(x):
    return lax.all_to_all(x, IN_PLANE, split_axis=0, concat_axis=0, tiled=True)


def upward(x, by):
    size = lax.axis_size("plane")
    return lax.ppermute(x, "plane", [(i, i + by) for i in range(size - by)])


def unpack(x):
    parts, tokens, width = x.shape
    return x.transpose(1, 0, 2).reshape(tokens, parts * width)


def shards(query_local, key_local, value_local, labels, query_global, key_global, value_global):
    planes = lax.axis_size("plane")
    plane = lax.axis_index("plane")
    parts = lax.axis_size("row") * lax.axis_size("head")
    spot = lax.axis_index("row") * lax.axis_size("head") + lax.axis_index("head")
    tokens = query_local.shape[0]
    width = query_local.shape[1] // parts
    members = width // HEAD
    rows = parts * tokens
    dtype = query_local.dtype
    local_back = min(planes - 1, -(-(STRETCH - 1) // rows))

    packed = jax.ShapeDtypeStruct((parts, 4, tokens, HEAD), dtype)
    pack = vmem_call(pack_body, packed, 4, nbytes=16 * key_local.size)
    pack = pack(key_local, value_local, key_global, value_global)
    own = exchange(pack)
    local_blocks, global_blocks = [own], [own]
    for d in range(1, planes):
        if d == 1:
            came = upward(own, 1)
            local_blocks.append(came)
            global_blocks.append(came)
        elif d == 2:
            if d <= local_back:
                local_blocks.append(upward(came[:, :2], 1))
            global_blocks.append(upward(came[:, 2:], 1))
        else:
            if d <= local_back:
                local_blocks.append(upward(local_blocks[d - 3][:, :2], 3))
            source = global_blocks[d - 3]
            global_blocks.append(upward(source[:, source.shape[1] - 2 :], 3))

    first = spot * tokens
    where = jnp.stack([plane, first]).astype(jnp.int32)
    bases = rope_tables(planes, rows)
    steps = rope_tables(rows, 1)
    turn = jnp.asarray(np.roll(np.eye(HEAD), HEAD // 2, axis=1), dtype)
    own_pos = plane * rows + first + jnp.arange(tokens, dtype=jnp.int32)
    temper = 1.0 + temper_slope * jnp.log(((own_pos + 1) // temper_floor + 1).astype(jnp.float32))
    temper = jnp.broadcast_to(temper[:, None], (tokens, HEAD))
    packed = jax.ShapeDtypeStruct((parts, 2, tokens, width), dtype)
    pack = vmem_call(pack_query_body, packed, 8, nbytes=8 * query_local.size, flops=2 * HEAD * query_local.size, smem=1)
    pack = pack(where, query_local, query_global, *bases, *steps, turn, temper)
    queries = exchange(pack)

    out_shape = jax.ShapeDtypeStruct((parts, tokens, width), dtype)
    pair_flops = 2 * 3 * rows * rows * HEAD * members
    local_out = vmem_call(
        functools.partial(local_body, local_back),
        out_shape,
        7 + local_back + 1,
        flops=pair_flops * (local_back + 1),
        nbytes=4 * rows * width * 2,
        exps=rows * rows * members * (local_back + 1),
        scratch=[
            pltpu.VMEM(((local_back + 1) * rows, 2 * HEAD), dtype),
            pltpu.VMEM(((local_back + 1) * rows, 2 * HEAD), dtype),
        ],
        smem=1,
    )(where, queries, labels[None, :], *bases, *steps, turn, *local_blocks)
    local_heads = exchange(local_out)
    global_out = vmem_call(
        functools.partial(global_body, planes),
        out_shape,
        1 + planes,
        flops=pair_flops * planes,
        nbytes=4 * rows * width * 2,
        exps=rows * rows * members * planes,
        scratch=[pltpu.VMEM((planes * rows, HEAD), dtype), pltpu.VMEM((planes * rows, 2 * HEAD), dtype)],
        smem=1,
    )(where, queries, *global_blocks)
    global_heads = exchange(global_out)
    return unpack(local_heads), unpack(global_heads)


def solution(mesh):
    ctx, head = mesh.shape["ctx"], mesh.shape["head"]

    def run(*args):
        key_heads = args[1].shape[1] // HEAD
        row = max(1, key_heads // head)
        grid = Mesh(mesh.devices.reshape(ctx // row, row, head), ("plane", "row", "head"))
        spread = P(("plane", "row", "head"), None)
        return jax.shard_map(
            shards,
            mesh=grid,
            in_specs=(spread, spread, spread, P(), spread, spread, spread),
            out_specs=(spread, spread),
            check_vma=False,
        )(*args)

    return run
```

```python
import functools

import jax
import jax.numpy as jnp
import numpy as np
from jax import lax
from jax.experimental import pallas as pl
from jax.experimental.pallas import tpu as pltpu
from jax.sharding import Mesh
from jax.sharding import PartitionSpec as P


HEAD = 128
STRETCH = 768

rope_base = 500000.0
norm_epsilon = 1e-06
temper_floor = 8192
temper_slope = 0.1
masked_score = -1e30
log2e = 1.4426950408889634
far = 30000.0
near_bytes = 4 << 20

IN_PLANE = ("row", "head")


def rope_tables(count, step):
    half = HEAD // 2
    frequency = rope_base ** (-(np.arange(HEAD) % half) * 2.0 / HEAD)
    angles = (np.arange(count) * step)[:, None] * frequency[None, :]
    sign = np.where(np.arange(HEAD) < half, -1.0, 1.0)
    return jnp.asarray(np.cos(angles), jnp.float32), jnp.asarray(np.sin(angles) * sign, jnp.float32)


def turned(cos_base, sin_base, cos_row, sin_row):
    return cos_base * cos_row - sin_base * sin_row, sin_base * cos_row + cos_base * sin_row


def rotated_unit(x, turn, cosine, sine):
    swapped = jnp.dot(x, turn, preferred_element_type=jnp.float32)
    y = x.astype(jnp.float32) * cosine + swapped * sine
    return y * lax.rsqrt(jnp.mean(y * y, axis=-1, keepdims=True) + norm_epsilon)


def vmem_call(body, out_shapes, n_in, flops=0, nbytes=0, exps=0, scratch=(), smem=0):
    return pl.pallas_call(
        body,
        out_shape=out_shapes,
        in_specs=[pl.BlockSpec(memory_space=pltpu.SMEM)] * smem
        + [pl.BlockSpec(memory_space=pltpu.VMEM)] * n_in,
        out_specs=jax.tree.map(lambda _: pl.BlockSpec(memory_space=pltpu.VMEM), out_shapes),
        scratch_shapes=list(scratch),
        cost_estimate=pl.CostEstimate(flops=flops, bytes_accessed=nbytes, transcendentals=exps),
    )


def pack_body(kl_ref, vl_ref, kg_ref, vg_ref, o_ref):
    for d in range(o_ref.shape[0]):
        for a, ref in enumerate((kl_ref, vl_ref, kg_ref, vg_ref)):
            o_ref[d, a] = ref[:, d * HEAD : (d + 1) * HEAD]


def pack_query_body(where_ref, ql_ref, qg_ref, cosb_ref, sinb_ref, cosr_ref, sinr_ref, turn_ref, temper_ref, o_ref):
    members = o_ref.shape[3] // HEAD
    tokens = ql_ref.shape[0]
    plane, first = where_ref[0], pl.multiple_of(where_ref[1], 16)
    mine = pl.ds(first, tokens)
    cosine, sine = turned(cosb_ref[pl.ds(plane, 1)], sinb_ref[pl.ds(plane, 1)], cosr_ref[mine], sinr_ref[mine])
    turn = turn_ref[...]
    for d in range(o_ref.shape[0]):
        for g in range(members):
            at = (d * members + g) * HEAD
            to = slice(g * HEAD, (g + 1) * HEAD)
            y = rotated_unit(ql_ref[:, at : at + HEAD], turn, cosine, sine)
            o_ref[d, 0, :, to] = y.astype(o_ref.dtype)
            z = qg_ref[:, at : at + HEAD].astype(jnp.float32) * temper_ref[...]
            o_ref[d, 1, :, to] = z.astype(o_ref.dtype)


def causal(rows):
    r = lax.broadcasted_iota(jnp.int32, (rows, rows), 0)
    c = lax.broadcasted_iota(jnp.int32, (rows, rows), 1)
    return c <= r


NT = (((1,), (1,)), ((), ()))


def take_values(v_ref, i, values, valid):
    rows = values.shape[0]
    v_ref[i * rows : (i + 1) * rows, :HEAD] = values
    ones = jnp.broadcast_to(jnp.where(valid, 1.0, 0.0), (rows, HEAD))
    v_ref[i * rows : (i + 1) * rows, HEAD:] = ones.astype(v_ref.dtype)


def divided(acc, dtype):
    return (acc[:, :HEAD] / acc[:, HEAD:]).astype(dtype)


def local_body(n_back, where_ref, *refs):
    q_ref, labels_ref, cosb_ref, sinb_ref, cosr_ref, sinr_ref, turn_ref = refs[:7]
    blocks = refs[7 : 7 + n_back + 1]
    o_ref, k_ref, v_ref = refs[7 + n_back + 1 :]
    parts, _, tokens, width = q_ref.shape
    rows = parts * tokens
    members = width // HEAD
    plane = where_ref[0]
    scale = log2e * HEAD**-0.5
    turn = turn_ref[...]
    lane = lax.broadcasted_iota(jnp.int32, (HEAD, rows), 0)
    for d in range(n_back + 1):
        behind = jnp.maximum(plane - d, 0)
        base = pl.ds(behind, 1)
        cosine, sine = turned(cosb_ref[base], sinb_ref[base], cosr_ref[...], sinr_ref[...])
        at = slice(d * rows, (d + 1) * rows)
        keys = blocks[d][:, 0].reshape(rows, HEAD)
        k_ref[at, :HEAD] = rotated_unit(keys, turn, cosine, sine).astype(k_ref.dtype)
        ids = labels_ref[:, pl.ds(pl.multiple_of(behind * rows, HEAD), rows)]
        same = jnp.where(lane == ids, 1.0, 0.0).T
        k_ref[at, HEAD:] = same.astype(k_ref.dtype)
        if d == 0:
            other = ((same - 1.0) * far).astype(k_ref.dtype)
        take_values(v_ref, d, blocks[d][:, 1].reshape(rows, HEAD), plane >= d)

    def member(g, carry):
        at = pl.multiple_of(g * HEAD, HEAD)
        q = jnp.concatenate([q_ref[:, 0, :, pl.ds(at, HEAD)].reshape(rows, HEAD), other], axis=1)
        scores = lax.dot_general(q, k_ref[...], NT, preferred_element_type=jnp.float32)
        weights = jnp.exp2(scores * scale)
        first = jnp.where(causal(rows), weights[:, :rows], 0.0)
        weights = jnp.concatenate([first, weights[:, rows:]], axis=1).astype(jnp.bfloat16)
        acc = jnp.dot(weights, v_ref[...], preferred_element_type=jnp.float32)
        o_ref[:, :, pl.ds(at, HEAD)] = divided(acc, o_ref.dtype).reshape(parts, tokens, HEAD)
        return carry

    lax.fori_loop(0, members, member, 0, unroll=True)


def global_body(n, where_ref, *refs):
    q_ref = refs[0]
    blocks = refs[1 : 1 + n]
    o_ref, k_ref, v_ref = refs[1 + n :]
    parts, _, tokens, width = q_ref.shape
    rows = parts * tokens
    members = width // HEAD
    plane = where_ref[0]
    scale = log2e * HEAD**-0.5
    groups = [(i, min(n, i + 4)) for i in range(0, n, 4)]
    for i in range(n):
        last = blocks[i].shape[1] - 1
        k_ref[i * rows : (i + 1) * rows] = blocks[i][:, last - 1].reshape(rows, HEAD)
        take_values(v_ref, i, blocks[i][:, last].reshape(rows, HEAD), plane >= i)

    def query(g):
        at = pl.multiple_of(g * HEAD, HEAD)
        return q_ref[:, 1, :, pl.ds(at, HEAD)].reshape(rows, HEAD)

    def put(g, acc):
        at = pl.multiple_of(g * HEAD, HEAD)
        o_ref[:, :, pl.ds(at, HEAD)] = divided(acc, o_ref.dtype).reshape(parts, tokens, HEAD)

    def scored(q, group):
        keys = k_ref[group[0] * rows : group[1] * rows]
        return lax.dot_general(q, keys, NT, preferred_element_type=jnp.float32) * scale

    def summed(weights, group):
        if group[0] == 0:
            first = jnp.where(causal(rows), weights[:, :rows], 0.0)
            weights = jnp.concatenate([first, weights[:, rows:]], axis=1)
        values = v_ref[group[0] * rows : group[1] * rows]
        return jnp.dot(weights.astype(jnp.bfloat16), values, preferred_element_type=jnp.float32)

    def plain(g, carry):
        low, high = carry
        q = query(g)
        acc = summed(jnp.exp2(scored(q, groups[0])), groups[0])
        for group in groups[1:]:
            acc = acc + summed(jnp.exp2(scored(q, group)), group)
        put(g, acc)
        totals = acc[:, HEAD:]
        low = jnp.minimum(low, jnp.min(totals, axis=0, keepdims=True))
        high = jnp.maximum(high, jnp.max(totals, axis=0, keepdims=True))
        return low, high

    ones = jnp.ones((1, HEAD), jnp.float32)
    low, high = lax.fori_loop(0, members, plain, (ones, ones), unroll=len(groups) == 1)
    safe = (jnp.min(low) > 2.0**-80) & (jnp.max(high) < 2.0**100)

    @pl.when(jnp.logical_not(safe))
    def _():
        def shifted(g, carry):
            q = query(g)
            peak, acc = None, None
            for group in groups:
                scores = scored(q, group)
                parts_of = []
                for i in range(group[0], group[1]):
                    part = scores[:, (i - group[0]) * rows : (i - group[0] + 1) * rows]
                    if i == 0:
                        part = jnp.where(causal(rows), part, masked_score)
                    else:
                        part = jnp.where(plane >= i, part, masked_score)
                    parts_of.append(part)
                scores = jnp.concatenate(parts_of, axis=1)
                top = jnp.max(scores, axis=1, keepdims=True)
                new_peak = top if peak is None else jnp.maximum(peak, top)
                if acc is not None:
                    acc = acc * jnp.exp2(peak - new_peak)
                peak = new_peak
                part = summed(jnp.exp2(scores - peak), group)
                acc = part if acc is None else acc + part
            put(g, acc)
            return carry

        lax.fori_loop(0, members, shifted, 0)


def near(*arrays):
    if sum(x.size * x.dtype.itemsize for x in arrays) > near_bytes:
        return arrays
    return tuple(pltpu.with_memory_space_constraint(x, pltpu.VMEM) for x in arrays)


def exchange(x):
    return lax.all_to_all(x, IN_PLANE, split_axis=0, concat_axis=0, tiled=True)


def upward(x, by):
    size = lax.axis_size("plane")
    return lax.ppermute(x, "plane", [(i, i + by) for i in range(size - by)])


def unpack(x):
    parts, tokens, width = x.shape
    return x.transpose(1, 0, 2).reshape(tokens, parts * width)


def shards(query_local, key_local, value_local, labels, query_global, key_global, value_global):
    planes = lax.axis_size("plane")
    plane = lax.axis_index("plane")
    parts = lax.axis_size("row") * lax.axis_size("head")
    spot = lax.axis_index("row") * lax.axis_size("head") + lax.axis_index("head")
    tokens = query_local.shape[0]
    width = query_local.shape[1] // parts
    members = width // HEAD
    rows = parts * tokens
    dtype = query_local.dtype
    local_back = min(planes - 1, -(-(STRETCH - 1) // rows))

    packed = jax.ShapeDtypeStruct((parts, 4, tokens, HEAD), dtype)
    pack = vmem_call(pack_body, packed, 4, nbytes=16 * key_local.size)
    pack = pack(key_local, value_local, key_global, value_global)
    own = exchange(pack)
    local_blocks, global_blocks = [own], [own]
    for d in range(1, planes):
        if d == 1:
            came = upward(own, 1)
            local_blocks.append(came)
            global_blocks.append(came)
        elif d == 2:
            if d <= local_back:
                local_blocks.append(upward(came[:, :2], 1))
            global_blocks.append(upward(came[:, 2:], 1))
        else:
            if d <= local_back:
                local_blocks.append(upward(local_blocks[d - 3][:, :2], 3))
            source = global_blocks[d - 3]
            global_blocks.append(upward(source[:, source.shape[1] - 2 :], 3))

    first = spot * tokens
    where = jnp.stack([plane, first]).astype(jnp.int32)
    bases = rope_tables(planes, rows)
    steps = rope_tables(rows, 1)
    turn = jnp.asarray(np.roll(np.eye(HEAD), HEAD // 2, axis=1), dtype)
    own_pos = plane * rows + first + jnp.arange(tokens, dtype=jnp.int32)
    temper = 1.0 + temper_slope * jnp.log(((own_pos + 1) // temper_floor + 1).astype(jnp.float32))
    temper = jnp.broadcast_to(temper[:, None], (tokens, HEAD))
    label_row = labels[None, :]
    packed = jax.ShapeDtypeStruct((parts, 2, tokens, width), dtype)
    pack = vmem_call(pack_query_body, packed, 8, nbytes=8 * query_local.size, flops=2 * HEAD * query_local.size, smem=1)
    pack = pack(where, query_local, query_global, *bases, *steps, turn, temper)
    queries = exchange(pack)

    kept = near(queries, *local_blocks, *global_blocks[1:])
    queries, local_blocks = kept[0], kept[1 : local_back + 2]
    global_blocks = [local_blocks[0], *kept[local_back + 2 :]]

    out_shape = jax.ShapeDtypeStruct((parts, tokens, width), dtype)
    pair_flops = 2 * 3 * rows * rows * HEAD * members
    local_out = vmem_call(
        functools.partial(local_body, local_back),
        out_shape,
        7 + local_back + 1,
        flops=pair_flops * (local_back + 1),
        nbytes=4 * rows * width * 2,
        exps=rows * rows * members * (local_back + 1),
        scratch=[
            pltpu.VMEM(((local_back + 1) * rows, 2 * HEAD), dtype),
            pltpu.VMEM(((local_back + 1) * rows, 2 * HEAD), dtype),
        ],
        smem=1,
    )(where, queries, label_row, *bases, *steps, turn, *local_blocks)
    local_heads = exchange(local_out)
    global_out = vmem_call(
        functools.partial(global_body, planes),
        out_shape,
        1 + planes,
        flops=pair_flops * planes,
        nbytes=4 * rows * width * 2,
        exps=rows * rows * members * planes,
        scratch=[pltpu.VMEM((planes * rows, HEAD), dtype), pltpu.VMEM((planes * rows, 2 * HEAD), dtype)],
        smem=1,
    )(where, queries, *global_blocks)
    global_heads = exchange(global_out)
    return unpack(local_heads), unpack(global_heads)


def solution(mesh):
    ctx, head = mesh.shape["ctx"], mesh.shape["head"]

    def run(*args):
        key_heads = args[1].shape[1] // HEAD
        row = max(1, key_heads // head)
        grid = Mesh(mesh.devices.reshape(ctx // row, row, head), ("plane", "row", "head"))
        spread = P(("plane", "row", "head"), None)
        return jax.shard_map(
            shards,
            mesh=grid,
            in_specs=(spread, spread, spread, P(), spread, spread, spread),
            out_specs=(spread, spread),
            check_vma=False,
        )(*args)

    return run
```

```python
import functools

import jax
import jax.numpy as jnp
import numpy as np
from jax import lax
from jax.experimental import pallas as pl
from jax.experimental.pallas import tpu as pltpu
from jax.sharding import Mesh
from jax.sharding import PartitionSpec as P


HEAD = 128
STRETCH = 768

rope_base = 500000.0
norm_epsilon = 1e-06
temper_floor = 8192
temper_slope = 0.1
masked_score = -1e30
log2e = 1.4426950408889634
far = 30000.0
near_bytes = 5 << 20
vmem_bytes = 40 << 20

IN_PLANE = ("row", "head")


def rope_tables(count, step):
    half = HEAD // 2
    frequency = rope_base ** (-(np.arange(HEAD) % half) * 2.0 / HEAD)
    angles = (np.arange(count) * step)[:, None] * frequency[None, :]
    sign = np.where(np.arange(HEAD) < half, -1.0, 1.0)
    return jnp.asarray(np.cos(angles), jnp.float32), jnp.asarray(np.sin(angles) * sign, jnp.float32)


def turned(cos_base, sin_base, cos_row, sin_row):
    return cos_base * cos_row - sin_base * sin_row, sin_base * cos_row + cos_base * sin_row


def rotated_unit(x, turn, cosine, sine):
    swapped = jnp.dot(x, turn, preferred_element_type=jnp.float32)
    y = x.astype(jnp.float32) * cosine + swapped * sine
    return y * lax.rsqrt(jnp.mean(y * y, axis=-1, keepdims=True) + norm_epsilon)


def vmem_call(body, out_shapes, n_in, flops=0, nbytes=0, exps=0, scratch=(), smem=0, limit=None):
    return pl.pallas_call(
        body,
        out_shape=out_shapes,
        in_specs=[pl.BlockSpec(memory_space=pltpu.SMEM)] * smem
        + [pl.BlockSpec(memory_space=pltpu.VMEM)] * n_in,
        out_specs=jax.tree.map(lambda _: pl.BlockSpec(memory_space=pltpu.VMEM), out_shapes),
        scratch_shapes=list(scratch),
        compiler_params=pltpu.CompilerParams(vmem_limit_bytes=limit),
        cost_estimate=pl.CostEstimate(flops=flops, bytes_accessed=nbytes, transcendentals=exps),
    )


def pack_body(kl_ref, vl_ref, kg_ref, vg_ref, o_ref):
    for d in range(o_ref.shape[0]):
        for a, ref in enumerate((kl_ref, vl_ref, kg_ref, vg_ref)):
            o_ref[d, a] = ref[:, d * HEAD : (d + 1) * HEAD]


def pack_query_body(where_ref, ql_ref, qg_ref, cosb_ref, sinb_ref, cosr_ref, sinr_ref, turn_ref, temper_ref, o_ref):
    members = o_ref.shape[3] // HEAD
    tokens = ql_ref.shape[0]
    plane, first = where_ref[0], pl.multiple_of(where_ref[1], 16)
    mine = pl.ds(first, tokens)
    cosine, sine = turned(cosb_ref[pl.ds(plane, 1)], sinb_ref[pl.ds(plane, 1)], cosr_ref[mine], sinr_ref[mine])
    turn = turn_ref[...]
    for d in range(o_ref.shape[0]):
        for g in range(members):
            at = (d * members + g) * HEAD
            to = slice(g * HEAD, (g + 1) * HEAD)
            y = rotated_unit(ql_ref[:, at : at + HEAD], turn, cosine, sine)
            o_ref[d, 0, :, to] = y.astype(o_ref.dtype)
            z = qg_ref[:, at : at + HEAD].astype(jnp.float32) * temper_ref[...]
            o_ref[d, 1, :, to] = z.astype(o_ref.dtype)


def causal(rows):
    r = lax.broadcasted_iota(jnp.int32, (rows, rows), 0)
    c = lax.broadcasted_iota(jnp.int32, (rows, rows), 1)
    return c <= r


def masked(weights, rows):
    first = jnp.where(causal(rows), weights[:, :rows], 0.0)
    if weights.shape[1] == rows:
        return first
    return jnp.concatenate([first, weights[:, rows:]], axis=1)


NT = (((1,), (1,)), ((), ()))


def take_values(v_ref, i, values, valid):
    rows = values.shape[0]
    v_ref[i * rows : (i + 1) * rows, :HEAD] = values
    ones = jnp.broadcast_to(jnp.where(valid, 1.0, 0.0), (rows, HEAD))
    v_ref[i * rows : (i + 1) * rows, HEAD:] = ones.astype(v_ref.dtype)


def same_stretch(labels_ref, behind, rows):
    ids = labels_ref[:, pl.ds(pl.multiple_of(behind * rows, HEAD), rows)]
    return jnp.where(lax.broadcasted_iota(jnp.int32, (HEAD, rows), 0) == ids, 1.0, 0.0).T


def take_local(shared, plane, distances, blocks, k_ref, v_ref):
    labels_ref, cosb_ref, sinb_ref, cosr_ref, sinr_ref, turn_ref = shared
    turn = turn_ref[...]
    for i, d in enumerate(distances):
        rows = k_ref.shape[0] // len(distances)
        behind = jnp.maximum(plane - d, 0)
        base = pl.ds(behind, 1)
        cosine, sine = turned(cosb_ref[base], sinb_ref[base], cosr_ref[...], sinr_ref[...])
        at = slice(i * rows, (i + 1) * rows)
        keys = blocks[i][:, 0].reshape(rows, HEAD)
        k_ref[at, :HEAD] = rotated_unit(keys, turn, cosine, sine).astype(k_ref.dtype)
        k_ref[at, HEAD:] = same_stretch(labels_ref, behind, rows).astype(k_ref.dtype)
        take_values(v_ref, i, blocks[i][:, 1].reshape(rows, HEAD), plane >= d)


def take_global(plane, distances, blocks, k_ref, v_ref):
    for i, d in enumerate(distances):
        rows = k_ref.shape[0] // len(distances)
        last = blocks[i].shape[1] - 1
        k_ref[i * rows : (i + 1) * rows] = blocks[i][:, last - 1].reshape(rows, HEAD)
        take_values(v_ref, i, blocks[i][:, last].reshape(rows, HEAD), plane >= d)


def query_of(q_ref, layer, g):
    parts, _, tokens, _ = q_ref.shape
    at = pl.multiple_of(g * HEAD, HEAD)
    return q_ref[:, layer, :, pl.ds(at, HEAD)].reshape(parts * tokens, HEAD)


def summed(q, k_ref, v_ref, rows, own):
    acc = None
    for at in range(0, k_ref.shape[0], 4 * rows):
        used = slice(at, min(k_ref.shape[0], at + 4 * rows))
        scores = lax.dot_general(q, k_ref[used], NT, preferred_element_type=jnp.float32)
        weights = jnp.exp2(scores * (log2e * HEAD**-0.5))
        if own and at == 0:
            weights = masked(weights, rows)
        part = jnp.dot(weights.astype(jnp.bfloat16), v_ref[used], preferred_element_type=jnp.float32)
        acc = part if acc is None else acc + part
    return acc


def early_body(n_near, where_ref, *refs):
    q_ref, *shared = refs[:7]
    blocks = refs[7 : 7 + n_near]
    lacc_ref, gacc_ref, lk_ref, lv_ref, gk_ref, gv_ref = refs[7 + n_near :]
    members, rows, _ = lacc_ref.shape
    plane = where_ref[0]
    take_local(shared, plane, range(n_near), blocks, lk_ref, lv_ref)
    take_global(plane, range(n_near), blocks, gk_ref, gv_ref)
    other = ((same_stretch(shared[0], plane, rows) - 1.0) * far).astype(lk_ref.dtype)

    def member(g, carry):
        q = jnp.concatenate([query_of(q_ref, 0, g), other], axis=1)
        lacc_ref[g] = summed(q, lk_ref, lv_ref, rows, True)
        gacc_ref[g] = summed(query_of(q_ref, 1, g), gk_ref, gv_ref, rows, True)
        return carry

    lax.fori_loop(0, members, member, 0, unroll=True)


def late_body(n_near, local_back, n, where_ref, *refs):
    q_ref, *shared = refs[:7]
    blocks = refs[7 : 7 + n]
    lacc_ref, gacc_ref, o_ref, lk_ref, lv_ref, gk_ref, gv_ref, allk_ref, allv_ref = refs[7 + n :]
    parts, _, tokens, _ = q_ref.shape
    members, rows, _ = lacc_ref.shape
    plane = where_ref[0]
    local_far = range(n_near, local_back + 1)
    take_local(shared, plane, local_far, [blocks[d] for d in local_far], lk_ref, lv_ref)
    take_global(plane, range(n_near, n), blocks[n_near:], gk_ref, gv_ref)
    other = ((same_stretch(shared[0], plane, rows) - 1.0) * far).astype(lk_ref.dtype)

    def put(g, layer, acc):
        at = pl.multiple_of(g * HEAD, HEAD)
        out = (acc[:, :HEAD] / acc[:, HEAD:]).astype(o_ref.dtype)
        o_ref[:, layer, :, pl.ds(at, HEAD)] = out.reshape(parts, tokens, HEAD)

    def member(g, carry):
        low, high = carry
        q = jnp.concatenate([query_of(q_ref, 0, g), other], axis=1)
        put(g, 0, lacc_ref[g] + summed(q, lk_ref, lv_ref, rows, False))
        acc = gacc_ref[g] + summed(query_of(q_ref, 1, g), gk_ref, gv_ref, rows, False)
        put(g, 1, acc)
        totals = acc[:, HEAD:]
        low = jnp.minimum(low, jnp.min(totals, axis=0, keepdims=True))
        high = jnp.maximum(high, jnp.max(totals, axis=0, keepdims=True))
        return low, high

    ones = jnp.ones((1, HEAD), jnp.float32)
    low, high = lax.fori_loop(0, members, member, (ones, ones), unroll=n <= 4)
    safe = (jnp.min(low) > 2.0**-80) & (jnp.max(high) < 2.0**100)

    @pl.when(jnp.logical_not(safe))
    def _():
        take_global(plane, range(n), blocks, allk_ref, allv_ref)

        def shifted(g, carry):
            q = query_of(q_ref, 1, g)
            peak, acc = None, None
            for first in range(0, n, 4):
                group = range(first, min(n, first + 4))
                used = slice(group[0] * rows, (group[-1] + 1) * rows)
                scores = lax.dot_general(q, allk_ref[used], NT, preferred_element_type=jnp.float32)
                scores = scores * (log2e * HEAD**-0.5)
                pieces = []
                for i in group:
                    piece = scores[:, (i - first) * rows : (i - first + 1) * rows]
                    allowed = causal(rows) if i == 0 else plane >= i
                    pieces.append(jnp.where(allowed, piece, masked_score))
                scores = jnp.concatenate(pieces, axis=1)
                top = jnp.max(scores, axis=1, keepdims=True)
                new_peak = top if peak is None else jnp.maximum(peak, top)
                if acc is not None:
                    acc = acc * jnp.exp2(peak - new_peak)
                peak = new_peak
                weights = jnp.exp2(scores - peak).astype(jnp.bfloat16)
                part = jnp.dot(weights, allv_ref[used], preferred_element_type=jnp.float32)
                acc = part if acc is None else acc + part
            put(g, 1, acc)
            return carry

        lax.fori_loop(0, members, shifted, 0)


def near(*arrays):
    if sum(x.size * x.dtype.itemsize for x in arrays) > near_bytes:
        return arrays
    return tuple(pltpu.with_memory_space_constraint(x, pltpu.VMEM) for x in arrays)


def exchange(x):
    return lax.all_to_all(x, IN_PLANE, split_axis=0, concat_axis=0, tiled=True)


def upward(x, by):
    size = lax.axis_size("plane")
    return lax.ppermute(x, "plane", [(i, i + by) for i in range(size - by)])


def unpack(x):
    parts, tokens, width = x.shape
    return x.transpose(1, 0, 2).reshape(tokens, parts * width)


def shards(query_local, key_local, value_local, labels, query_global, key_global, value_global):
    planes = lax.axis_size("plane")
    plane = lax.axis_index("plane")
    parts = lax.axis_size("row") * lax.axis_size("head")
    spot = lax.axis_index("row") * lax.axis_size("head") + lax.axis_index("head")
    tokens = query_local.shape[0]
    width = query_local.shape[1] // parts
    members = width // HEAD
    rows = parts * tokens
    dtype = query_local.dtype
    local_back = min(planes - 1, -(-(STRETCH - 1) // rows))

    packed = jax.ShapeDtypeStruct((parts, 4, tokens, HEAD), dtype)
    pack = vmem_call(pack_body, packed, 4, nbytes=16 * key_local.size)
    pack = pack(key_local, value_local, key_global, value_global)
    own = exchange(pack)
    blocks = [own]
    for d in range(1, planes):
        step = 1 if d < 3 else 3
        source = blocks[d - step]
        if d > local_back:
            source = source[:, source.shape[1] - 2 :]
        blocks.append(upward(source, step))

    first = spot * tokens
    where = jnp.stack([plane, first]).astype(jnp.int32)
    bases = rope_tables(planes, rows)
    steps = rope_tables(rows, 1)
    turn = jnp.asarray(np.roll(np.eye(HEAD), HEAD // 2, axis=1), dtype)
    own_pos = plane * rows + first + jnp.arange(tokens, dtype=jnp.int32)
    temper = 1.0 + temper_slope * jnp.log(((own_pos + 1) // temper_floor + 1).astype(jnp.float32))
    temper = jnp.broadcast_to(temper[:, None], (tokens, HEAD))
    label_row = labels[None, :]
    packed = jax.ShapeDtypeStruct((parts, 2, tokens, width), dtype)
    pack = vmem_call(pack_query_body, packed, 8, nbytes=8 * query_local.size, flops=2 * HEAD * query_local.size, smem=1)
    pack = pack(where, query_local, query_global, *bases, *steps, turn, temper)
    queries = exchange(pack)

    n_near = min(2, planes)
    queries, *blocks = near(queries, *blocks)
    shared = (label_row, *bases, *steps, turn)
    sums = jax.ShapeDtypeStruct((members, rows, 2 * HEAD), jnp.float32)
    unit = 2 * 3 * rows * rows * HEAD * members

    def scratch(count, columns):
        return pltpu.VMEM((max(1, count) * rows, columns), dtype)

    early = vmem_call(
        functools.partial(early_body, n_near),
        (sums, sums),
        7 + n_near,
        flops=unit * 2 * n_near,
        nbytes=8 * rows * width,
        exps=rows * rows * members * 2 * n_near,
        scratch=[scratch(n_near, 2 * HEAD)] * 2 + [scratch(n_near, HEAD), scratch(n_near, 2 * HEAD)],
        smem=1,
        limit=vmem_bytes,
    )(where, queries, *shared, *blocks[:n_near])
    early = near(*early)
    out = vmem_call(
        functools.partial(late_body, n_near, local_back, planes),
        jax.ShapeDtypeStruct((parts, 2, tokens, width), dtype),
        7 + planes + 2,
        flops=unit * (planes + local_back + 1 - 2 * n_near),
        nbytes=8 * rows * width,
        exps=rows * rows * members * (planes + local_back + 1 - 2 * n_near),
        scratch=[scratch(local_back + 1 - n_near, 2 * HEAD)] * 2
        + [scratch(planes - n_near, HEAD), scratch(planes - n_near, 2 * HEAD)]
        + [scratch(planes, HEAD), scratch(planes, 2 * HEAD)],
        smem=1,
        limit=vmem_bytes,
    )(where, queries, *shared, *blocks, *early)
    heads = exchange(out)
    return unpack(heads[:, 0]), unpack(heads[:, 1])


def solution(mesh):
    ctx, head = mesh.shape["ctx"], mesh.shape["head"]

    def run(*args):
        key_heads = args[1].shape[1] // HEAD
        row = max(1, key_heads // head)
        grid = Mesh(mesh.devices.reshape(ctx // row, row, head), ("plane", "row", "head"))
        spread = P(("plane", "row", "head"), None)
        return jax.shard_map(
            shards,
            mesh=grid,
            in_specs=(spread, spread, spread, P(), spread, spread, spread),
            out_specs=(spread, spread),
            check_vma=False,
        )(*args)

    return run
```

```python
import functools

import jax
import jax.numpy as jnp
import numpy as np
from jax import lax
from jax.experimental import pallas as pl
from jax.experimental.pallas import tpu as pltpu
from jax.sharding import Mesh
from jax.sharding import PartitionSpec as P


HEAD = 128
STRETCH = 768

rope_base = 500000.0
norm_epsilon = 1e-06
temper_floor = 8192
temper_slope = 0.1
masked_score = -1e30
log2e = 1.4426950408889634
far = 30000.0
near_bytes = 6 << 20
vmem_bytes = 40 << 20

IN_PLANE = ("row", "head")


def rope_tables(count, step):
    half = HEAD // 2
    frequency = rope_base ** (-(np.arange(HEAD) % half) * 2.0 / HEAD)
    angles = (np.arange(count) * step)[:, None] * frequency[None, :]
    sign = np.where(np.arange(HEAD) < half, -1.0, 1.0)
    return jnp.asarray(np.cos(angles), jnp.float32), jnp.asarray(np.sin(angles) * sign, jnp.float32)


def turned(cos_base, sin_base, cos_row, sin_row):
    return cos_base * cos_row - sin_base * sin_row, sin_base * cos_row + cos_base * sin_row


def rotated_unit(x, turn, cosine, sine):
    swapped = jnp.dot(x, turn, preferred_element_type=jnp.float32)
    y = x.astype(jnp.float32) * cosine + swapped * sine
    return y * lax.rsqrt(jnp.mean(y * y, axis=-1, keepdims=True) + norm_epsilon)


def spot_of():
    return lax.axis_index("row") * lax.axis_size("head") + lax.axis_index("head")


def partner_orders(parts):
    return sorted(range(1, parts), key=lambda s: (s & 1, -s)) if parts > 1 else []


def vmem_call(body, out_shapes, n_in, flops=0, nbytes=0, exps=0, scratch=(), smem=0, limit=None):
    return pl.pallas_call(
        body,
        out_shape=out_shapes,
        in_specs=[pl.BlockSpec(memory_space=pltpu.SMEM)] * smem
        + [pl.BlockSpec(memory_space=pltpu.VMEM)] * n_in,
        out_specs=jax.tree.map(lambda _: pl.BlockSpec(memory_space=pltpu.VMEM), out_shapes),
        scratch_shapes=list(scratch),
        compiler_params=pltpu.CompilerParams(vmem_limit_bytes=limit),
        cost_estimate=pl.CostEstimate(flops=flops, bytes_accessed=nbytes, transcendentals=exps),
    )


def pack_body(kl_ref, vl_ref, kg_ref, vg_ref, o_ref):
    for d in range(o_ref.shape[0]):
        for a, ref in enumerate((kl_ref, vl_ref, kg_ref, vg_ref)):
            o_ref[d, a] = ref[:, d * HEAD : (d + 1) * HEAD]


def pack_query_body(ql_ref, qg_ref, cosb_ref, sinb_ref, cosr_ref, sinr_ref, turn_ref, temper_ref, *o_refs):
    tokens, width = ql_ref.shape[0], o_refs[0].shape[2]
    spot = spot_of()
    base, mine = pl.ds(lax.axis_index("plane"), 1), pl.ds(pl.multiple_of(spot * tokens, 16), tokens)
    cosine, sine = turned(cosb_ref[base], sinb_ref[base], cosr_ref[mine], sinr_ref[mine])
    turn = turn_ref[...]
    for s, o_ref in enumerate(o_refs):
        to = lax.bitwise_xor(spot, s)
        for g in range(width // HEAD):
            at = pl.ds(pl.multiple_of(to * width + g * HEAD, HEAD), HEAD)
            out = slice(g * HEAD, (g + 1) * HEAD)
            o_ref[0, :, out] = rotated_unit(ql_ref[:, at], turn, cosine, sine).astype(o_ref.dtype)
            o_ref[1, :, out] = (qg_ref[:, at].astype(jnp.float32) * temper_ref[...]).astype(o_ref.dtype)


def causal(rows):
    r = lax.broadcasted_iota(jnp.int32, (rows, rows), 0)
    c = lax.broadcasted_iota(jnp.int32, (rows, rows), 1)
    return c <= r


def masked(weights, rows):
    first = jnp.where(causal(rows), weights[:, :rows], 0.0)
    if weights.shape[1] == rows:
        return first
    return jnp.concatenate([first, weights[:, rows:]], axis=1)


NT = (((1,), (1,)), ((), ()))


def take_values(v_ref, i, values, valid):
    rows = values.shape[0]
    v_ref[i * rows : (i + 1) * rows, :HEAD] = values
    ones = jnp.broadcast_to(jnp.where(valid, 1.0, 0.0), (rows, HEAD))
    v_ref[i * rows : (i + 1) * rows, HEAD:] = ones.astype(v_ref.dtype)


def same_stretch(labels_ref, behind, rows):
    ids = labels_ref[:, pl.ds(pl.multiple_of(behind * rows, HEAD), rows)]
    return jnp.where(lax.broadcasted_iota(jnp.int32, (HEAD, rows), 0) == ids, 1.0, 0.0).T


def take_local(shared, plane, distances, blocks, k_ref, v_ref):
    labels_ref, cosb_ref, sinb_ref, cosr_ref, sinr_ref, turn_ref = shared
    turn = turn_ref[...]
    for i, d in enumerate(distances):
        rows = k_ref.shape[0] // len(distances)
        behind = jnp.maximum(plane - d, 0)
        base = pl.ds(behind, 1)
        cosine, sine = turned(cosb_ref[base], sinb_ref[base], cosr_ref[...], sinr_ref[...])
        at = slice(i * rows, (i + 1) * rows)
        keys = blocks[i][:, 0].reshape(rows, HEAD)
        k_ref[at, :HEAD] = rotated_unit(keys, turn, cosine, sine).astype(k_ref.dtype)
        k_ref[at, HEAD:] = same_stretch(labels_ref, behind, rows).astype(k_ref.dtype)
        take_values(v_ref, i, blocks[i][:, 1].reshape(rows, HEAD), plane >= d)


def take_global(plane, distances, blocks, k_ref, v_ref):
    for i, d in enumerate(distances):
        rows = k_ref.shape[0] // len(distances)
        last = blocks[i].shape[1] - 1
        k_ref[i * rows : (i + 1) * rows] = blocks[i][:, last - 1].reshape(rows, HEAD)
        take_values(v_ref, i, blocks[i][:, last].reshape(rows, HEAD), plane >= d)


def query_of(q_ref, layer, g):
    return q_ref[layer, :, pl.ds(pl.multiple_of(g * HEAD, HEAD), HEAD)]


def summed(q, k_ref, v_ref, rows, own):
    acc = None
    for at in range(0, k_ref.shape[0], 4 * rows):
        used = slice(at, min(k_ref.shape[0], at + 4 * rows))
        scores = lax.dot_general(q, k_ref[used], NT, preferred_element_type=jnp.float32)
        weights = jnp.exp2(scores * (log2e * HEAD**-0.5))
        if own and at == 0:
            weights = masked(weights, rows)
        part = jnp.dot(weights.astype(jnp.bfloat16), v_ref[used], preferred_element_type=jnp.float32)
        acc = part if acc is None else acc + part
    return acc


def early_body(n_near, *refs):
    shared, refs = refs[:6], refs[6:]
    parts = refs[0].shape[0]
    queries, blocks, refs = refs[n_near : n_near + parts], refs[:n_near], refs[n_near + parts :]
    q_ref, lacc_ref, gacc_ref, lk_ref, lv_ref, gk_ref, gv_ref = refs
    members, rows, _ = lacc_ref.shape
    tokens = rows // parts
    plane, spot = lax.axis_index("plane"), spot_of()
    for s, ref in enumerate(queries):
        at = pl.ds(pl.multiple_of(lax.bitwise_xor(spot, s) * tokens, 16), tokens)
        q_ref[:, at] = ref[...]
    take_local(shared, plane, range(n_near), blocks, lk_ref, lv_ref)
    take_global(plane, range(n_near), blocks, gk_ref, gv_ref)
    other = ((same_stretch(shared[0], plane, rows) - 1.0) * far).astype(lk_ref.dtype)

    def member(g, carry):
        q = jnp.concatenate([query_of(q_ref, 0, g), other], axis=1)
        lacc_ref[g] = summed(q, lk_ref, lv_ref, rows, True)
        gacc_ref[g] = summed(query_of(q_ref, 1, g), gk_ref, gv_ref, rows, True)
        return carry

    lax.fori_loop(0, members, member, 0, unroll=True)


def late_body(n_near, local_back, n, *refs):
    shared, refs = refs[:6], refs[6:]
    blocks, refs = refs[:n], refs[n:]
    parts = blocks[0].shape[0]
    q_ref, lacc_ref, gacc_ref = refs[:3]
    o_refs, refs = refs[3 : 3 + parts], refs[3 + parts :]
    out_ref, lk_ref, lv_ref, gk_ref, gv_ref, allk_ref, allv_ref = refs
    members, rows, _ = lacc_ref.shape
    tokens = rows // parts
    plane, spot = lax.axis_index("plane"), spot_of()
    local_far = range(n_near, local_back + 1)
    take_local(shared, plane, local_far, [blocks[d] for d in local_far], lk_ref, lv_ref)
    take_global(plane, range(n_near, n), blocks[n_near:], gk_ref, gv_ref)
    other = ((same_stretch(shared[0], plane, rows) - 1.0) * far).astype(lk_ref.dtype)

    def put(g, layer, acc):
        at = pl.multiple_of(g * HEAD, HEAD)
        out_ref[layer, :, pl.ds(at, HEAD)] = (acc[:, :HEAD] / acc[:, HEAD:]).astype(out_ref.dtype)

    def member(g, carry):
        low, high = carry
        q = jnp.concatenate([query_of(q_ref, 0, g), other], axis=1)
        put(g, 0, lacc_ref[g] + summed(q, lk_ref, lv_ref, rows, False))
        acc = gacc_ref[g] + summed(query_of(q_ref, 1, g), gk_ref, gv_ref, rows, False)
        put(g, 1, acc)
        totals = acc[:, HEAD:]
        low = jnp.minimum(low, jnp.min(totals, axis=0, keepdims=True))
        high = jnp.maximum(high, jnp.max(totals, axis=0, keepdims=True))
        return low, high

    ones = jnp.ones((1, HEAD), jnp.float32)
    low, high = lax.fori_loop(0, members, member, (ones, ones), unroll=n <= 4)
    safe = (jnp.min(low) > 2.0**-80) & (jnp.max(high) < 2.0**100)

    @pl.when(jnp.logical_not(safe))
    def _():
        take_global(plane, range(n), blocks, allk_ref, allv_ref)

        def shifted(g, carry):
            q = query_of(q_ref, 1, g)
            peak, acc = None, None
            for first in range(0, n, 4):
                group = range(first, min(n, first + 4))
                used = slice(group[0] * rows, (group[-1] + 1) * rows)
                scores = lax.dot_general(q, allk_ref[used], NT, preferred_element_type=jnp.float32)
                scores = scores * (log2e * HEAD**-0.5)
                pieces = []
                for i in group:
                    piece = scores[:, (i - first) * rows : (i - first + 1) * rows]
                    allowed = causal(rows) if i == 0 else plane >= i
                    pieces.append(jnp.where(allowed, piece, masked_score))
                scores = jnp.concatenate(pieces, axis=1)
                top = jnp.max(scores, axis=1, keepdims=True)
                new_peak = top if peak is None else jnp.maximum(peak, top)
                if acc is not None:
                    acc = acc * jnp.exp2(peak - new_peak)
                peak = new_peak
                weights = jnp.exp2(scores - peak).astype(jnp.bfloat16)
                part = jnp.dot(weights, allv_ref[used], preferred_element_type=jnp.float32)
                acc = part if acc is None else acc + part
            put(g, 1, acc)
            return carry

        lax.fori_loop(0, members, shifted, 0)

    for s, o_ref in enumerate(o_refs):
        at = pl.ds(pl.multiple_of(lax.bitwise_xor(spot, s) * tokens, 16), tokens)
        o_ref[...] = out_ref[:, at]


def near(*arrays):
    if sum(x.size * x.dtype.itemsize for x in arrays) > near_bytes:
        return arrays
    return tuple(pltpu.with_memory_space_constraint(x, pltpu.VMEM) for x in arrays)


def exchange(x):
    return lax.all_to_all(x, IN_PLANE, split_axis=0, concat_axis=0, tiled=True)


def upward(x, by):
    size = lax.axis_size("plane")
    return lax.ppermute(x, "plane", [(i, i + by) for i in range(size - by)])


def unpack_body(parts, *refs):
    x_refs, o_refs, sems = refs[:parts], refs[parts:-1], refs[-1]
    width = x_refs[0].shape[2]
    spot = spot_of()
    copies = []
    for s, x_ref in enumerate(x_refs):
        at = pl.ds(pl.multiple_of(lax.bitwise_xor(spot, s) * width, HEAD), width)
        for layer, o_ref in enumerate(o_refs):
            copies.append(pltpu.make_async_copy(x_ref.at[layer], o_ref.at[:, at], sems.at[s, layer]))
    for copy in copies:
        copy.start()
    for copy in copies:
        copy.wait()


def unpack(pieces):
    parts = len(pieces)
    layers, tokens, width = pieces[0].shape
    shape = jax.ShapeDtypeStruct((tokens, parts * width), pieces[0].dtype)
    return pl.pallas_call(
        functools.partial(unpack_body, parts),
        out_shape=(shape,) * layers,
        in_specs=[pl.BlockSpec(memory_space=pltpu.VMEM)] * parts,
        out_specs=(pl.BlockSpec(memory_space=pl.ANY),) * layers,
        scratch_shapes=[pltpu.SemaphoreType.DMA((parts, layers))],
        cost_estimate=pl.CostEstimate(flops=0, bytes_accessed=4 * parts * pieces[0].size, transcendentals=0),
    )(*pieces)


def swapped(pieces):
    parts = len(pieces)
    came = [pieces[0]] * parts
    for s in partner_orders(parts):
        came[s] = lax.ppermute(pieces[s], IN_PLANE, [(i, i ^ s) for i in range(parts)])
    return came


def shards(query_local, key_local, value_local, labels, query_global, key_global, value_global):
    planes = lax.axis_size("plane")
    plane = lax.axis_index("plane")
    parts = lax.axis_size("row") * lax.axis_size("head")
    spot = lax.axis_index("row") * lax.axis_size("head") + lax.axis_index("head")
    tokens = query_local.shape[0]
    width = query_local.shape[1] // parts
    members = width // HEAD
    rows = parts * tokens
    dtype = query_local.dtype
    local_back = min(planes - 1, -(-(STRETCH - 1) // rows))

    packed = jax.ShapeDtypeStruct((parts, 4, tokens, HEAD), dtype)
    pack = vmem_call(pack_body, packed, 4, nbytes=16 * key_local.size)
    pack = pack(key_local, value_local, key_global, value_global)
    own = exchange(pack)
    blocks = [own]
    for d in range(1, planes):
        step = 1 if d < 3 else 3
        source = blocks[d - step]
        if d > local_back:
            source = source[:, source.shape[1] - 2 :]
        blocks.append(upward(source, step))

    bases = rope_tables(planes, rows)
    steps = rope_tables(rows, 1)
    turn = jnp.asarray(np.roll(np.eye(HEAD), HEAD // 2, axis=1), dtype)
    own_pos = plane * rows + spot * tokens + jnp.arange(tokens, dtype=jnp.int32)
    temper = 1.0 + temper_slope * jnp.log(((own_pos + 1) // temper_floor + 1).astype(jnp.float32))
    temper = jnp.broadcast_to(temper[:, None], (tokens, HEAD))
    label_row = labels[None, :]
    piece = jax.ShapeDtypeStruct((2, tokens, width), dtype)
    pack = vmem_call(
        pack_query_body, (piece,) * parts, 8, nbytes=8 * query_local.size, flops=2 * HEAD * query_local.size
    )
    queries = pack(query_local, query_global, *bases, *steps, turn, temper)
    queries = swapped(queries)

    n_near = min(2, planes)
    kept = near(*queries[1:], *blocks)
    queries, blocks = (queries[0], *kept[: parts - 1]), kept[parts - 1 :]
    shared = (label_row, *bases, *steps, turn)
    placed = jax.ShapeDtypeStruct((2, rows, width), dtype)
    sums = jax.ShapeDtypeStruct((members, rows, 2 * HEAD), jnp.float32)
    unit = 2 * 3 * rows * rows * HEAD * members

    def scratch(count, columns):
        return pltpu.VMEM((max(1, count) * rows, columns), dtype)

    early = vmem_call(
        functools.partial(early_body, n_near),
        (placed, sums, sums),
        6 + n_near + parts,
        flops=unit * 2 * n_near,
        nbytes=8 * rows * width,
        exps=rows * rows * members * 2 * n_near,
        scratch=[scratch(n_near, 2 * HEAD)] * 2 + [scratch(n_near, HEAD), scratch(n_near, 2 * HEAD)],
        limit=vmem_bytes,
    )(*shared, *blocks[:n_near], *queries)
    early = near(*early)
    out = vmem_call(
        functools.partial(late_body, n_near, local_back, planes),
        (piece,) * parts,
        6 + planes + 3,
        flops=unit * (planes + local_back + 1 - 2 * n_near),
        nbytes=8 * rows * width,
        exps=rows * rows * members * (planes + local_back + 1 - 2 * n_near),
        scratch=[pltpu.VMEM((2, rows, width), dtype)]
        + [scratch(local_back + 1 - n_near, 2 * HEAD)] * 2
        + [scratch(planes - n_near, HEAD), scratch(planes - n_near, 2 * HEAD)]
        + [scratch(planes, HEAD), scratch(planes, 2 * HEAD)],
        limit=vmem_bytes,
    )(*shared, *blocks, *early)
    return unpack(near(*swapped(out)))


def solution(mesh):
    ctx, head = mesh.shape["ctx"], mesh.shape["head"]

    def run(*args):
        key_heads = args[1].shape[1] // HEAD
        row = max(1, key_heads // head)
        grid = Mesh(mesh.devices.reshape(ctx // row, row, head), ("plane", "row", "head"))
        spread = P(("plane", "row", "head"), None)
        return jax.shard_map(
            shards,
            mesh=grid,
            in_specs=(spread, spread, spread, P(), spread, spread, spread),
            out_specs=(spread, spread),
            check_vma=False,
        )(*args)

    return run
```

```python
import functools

import jax
import jax.numpy as jnp
import numpy as np
from jax import lax
from jax.experimental import pallas as pl
from jax.experimental.pallas import tpu as pltpu
from jax.sharding import Mesh
from jax.sharding import PartitionSpec as P


HEAD = 128
STRETCH = 768

rope_base = 500000.0
norm_epsilon = 1e-06
temper_floor = 8192
temper_slope = 0.1
masked_score = -1e30
log2e = 1.4426950408889634
far = 30000.0
near_bytes = 6 << 20
vmem_bytes = 40 << 20

IN_PLANE = ("row", "head")


def rope_tables(count, step):
    half = HEAD // 2
    frequency = rope_base ** (-(np.arange(HEAD) % half) * 2.0 / HEAD)
    angles = (np.arange(count) * step)[:, None] * frequency[None, :]
    sign = np.where(np.arange(HEAD) < half, -1.0, 1.0)
    return jnp.asarray(np.cos(angles), jnp.float32), jnp.asarray(np.sin(angles) * sign, jnp.float32)


def turned(cos_base, sin_base, cos_row, sin_row):
    return cos_base * cos_row - sin_base * sin_row, sin_base * cos_row + cos_base * sin_row


def rotated_unit(x, turn, cosine, sine):
    swapped = jnp.dot(x, turn, preferred_element_type=jnp.float32)
    y = x.astype(jnp.float32) * cosine + swapped * sine
    return y * lax.rsqrt(jnp.mean(y * y, axis=-1, keepdims=True) + norm_epsilon)


def spot_of():
    return lax.axis_index("row") * lax.axis_size("head") + lax.axis_index("head")


def partner_orders(parts):
    return sorted(range(1, parts), key=lambda s: (s & 1, -s)) if parts > 1 else []


def vmem_call(body, out_shapes, n_in, flops=0, nbytes=0, exps=0, scratch=(), smem=0, limit=None):
    return pl.pallas_call(
        body,
        out_shape=out_shapes,
        in_specs=[pl.BlockSpec(memory_space=pltpu.SMEM)] * smem
        + [pl.BlockSpec(memory_space=pltpu.VMEM)] * n_in,
        out_specs=jax.tree.map(lambda _: pl.BlockSpec(memory_space=pltpu.VMEM), out_shapes),
        scratch_shapes=list(scratch),
        compiler_params=pltpu.CompilerParams(vmem_limit_bytes=limit),
        cost_estimate=pl.CostEstimate(flops=flops, bytes_accessed=nbytes, transcendentals=exps),
    )


def pack_body(kl_ref, vl_ref, kg_ref, vg_ref, o_ref):
    for d in range(o_ref.shape[0]):
        for a, ref in enumerate((kl_ref, vl_ref, kg_ref, vg_ref)):
            o_ref[d, a] = ref[:, d * HEAD : (d + 1) * HEAD]


def pack_query_body(ql_ref, qg_ref, cosb_ref, sinb_ref, cosr_ref, sinr_ref, turn_ref, temper_ref, *o_refs):
    tokens, width = ql_ref.shape[0], o_refs[0].shape[2]
    spot = spot_of()
    base, mine = pl.ds(lax.axis_index("plane"), 1), pl.ds(pl.multiple_of(spot * tokens, 16), tokens)
    cosine, sine = turned(cosb_ref[base], sinb_ref[base], cosr_ref[mine], sinr_ref[mine])
    turn = turn_ref[...]
    for s, o_ref in enumerate(o_refs):
        to = lax.bitwise_xor(spot, s)
        for g in range(width // HEAD):
            at = pl.ds(pl.multiple_of(to * width + g * HEAD, HEAD), HEAD)
            out = slice(g * HEAD, (g + 1) * HEAD)
            o_ref[0, :, out] = rotated_unit(ql_ref[:, at], turn, cosine, sine).astype(o_ref.dtype)
            o_ref[1, :, out] = (qg_ref[:, at].astype(jnp.float32) * temper_ref[...]).astype(o_ref.dtype)


def causal(rows):
    r = lax.broadcasted_iota(jnp.int32, (rows, rows), 0)
    c = lax.broadcasted_iota(jnp.int32, (rows, rows), 1)
    return c <= r


def masked(weights, rows):
    first = jnp.where(causal(rows), weights[:, :rows], 0.0)
    if weights.shape[1] == rows:
        return first
    return jnp.concatenate([first, weights[:, rows:]], axis=1)


NT = (((1,), (1,)), ((), ()))


def take_values(v_ref, i, values, valid):
    rows = values.shape[0]
    v_ref[i * rows : (i + 1) * rows, :HEAD] = values
    ones = jnp.broadcast_to(jnp.where(valid, 1.0, 0.0), (rows, HEAD))
    v_ref[i * rows : (i + 1) * rows, HEAD:] = ones.astype(v_ref.dtype)


def same_stretch(labels_ref, behind, rows):
    ids = labels_ref[:, pl.ds(pl.multiple_of(behind * rows, HEAD), rows)]
    return jnp.where(lax.broadcasted_iota(jnp.int32, (HEAD, rows), 0) == ids, 1.0, 0.0).T


def take_local(shared, plane, distances, blocks, same, k_ref, v_ref):
    cosb_ref, sinb_ref, cosr_ref, sinr_ref, turn_ref = shared
    turn = turn_ref[...]
    for i, d in enumerate(distances):
        rows = k_ref.shape[0] // len(distances)
        base = pl.ds(jnp.maximum(plane - d, 0), 1)
        cosine, sine = turned(cosb_ref[base], sinb_ref[base], cosr_ref[...], sinr_ref[...])
        at = slice(i * rows, (i + 1) * rows)
        keys = blocks[d][:, 0].reshape(rows, HEAD)
        k_ref[at, :HEAD] = rotated_unit(keys, turn, cosine, sine).astype(k_ref.dtype)
        k_ref[at, HEAD:] = same[i].astype(k_ref.dtype)
        take_values(v_ref, i, blocks[d][:, 1].reshape(rows, HEAD), plane >= d)


def take_global(plane, distances, blocks, k_ref, v_ref):
    for i, d in enumerate(distances):
        rows = k_ref.shape[0] // len(distances)
        last = blocks[d].shape[1] - 1
        k_ref[i * rows : (i + 1) * rows] = blocks[d][:, last - 1].reshape(rows, HEAD)
        take_values(v_ref, i, blocks[d][:, last].reshape(rows, HEAD), plane >= d)


def query_of(q_ref, layer, g):
    return q_ref[layer, :, pl.ds(pl.multiple_of(g * HEAD, HEAD), HEAD)]


def summed(q, k_ref, v_ref, rows, own):
    acc = None
    for at in range(0, k_ref.shape[0], 4 * rows):
        used = slice(at, min(k_ref.shape[0], at + 4 * rows))
        scores = lax.dot_general(q, k_ref[used], NT, preferred_element_type=jnp.float32)
        weights = jnp.exp2(scores * (log2e * HEAD**-0.5))
        if own and at == 0:
            weights = masked(weights, rows)
        part = jnp.dot(weights.astype(jnp.bfloat16), v_ref[used], preferred_element_type=jnp.float32)
        acc = part if acc is None else acc + part
    return acc


def early_body(plan, labels_ref, *refs):
    _, n_queries, local_near, local_far, global_near, _ = plan
    shared, refs = refs[:5], refs[5:]
    blocks = dict(zip(global_near, refs))
    queries, refs = refs[len(blocks) : len(blocks) + n_queries], refs[len(blocks) + n_queries :]
    q_ref, lacc_ref, gacc_ref, other_ref, same_ref, lk_ref, lv_ref, gk_ref, gv_ref = refs
    members, rows, _ = lacc_ref.shape
    tokens = rows // n_queries
    plane, spot = lax.axis_index("plane"), spot_of()
    for s, ref in enumerate(queries):
        at = pl.ds(pl.multiple_of(lax.bitwise_xor(spot, s) * tokens, 16), tokens)
        q_ref[:, at] = ref[...]
    same = [same_stretch(labels_ref, jnp.maximum(plane - d, 0), rows) for d in local_near]
    other = ((same[0] - 1.0) * far).astype(other_ref.dtype)
    other_ref[...] = other
    for i, d in enumerate(local_far):
        same_ref[i] = same_stretch(labels_ref, jnp.maximum(plane - d, 0), rows).astype(same_ref.dtype)
    take_local(shared, plane, local_near, blocks, same, lk_ref, lv_ref)
    take_global(plane, global_near, blocks, gk_ref, gv_ref)

    def member(g, carry):
        q = jnp.concatenate([query_of(q_ref, 0, g), other], axis=1)
        lacc_ref[g] = summed(q, lk_ref, lv_ref, rows, True)
        gacc_ref[g] = summed(query_of(q_ref, 1, g), gk_ref, gv_ref, rows, True)
        return carry

    lax.fori_loop(0, members, member, 0, unroll=True)


def late_body(plan, *refs):
    n, n_queries, _, local_far, _, global_far = plan
    shared, refs = refs[:5], refs[5:]
    blocks, refs = refs[:n], refs[n:]
    q_ref, lacc_ref, gacc_ref, other_ref, same_ref = refs[:5]
    o_refs, refs = refs[5 : 5 + n_queries], refs[5 + n_queries :]
    out_ref, lk_ref, lv_ref, gk_ref, gv_ref, allk_ref, allv_ref = refs
    members, rows, _ = lacc_ref.shape
    tokens = rows // n_queries
    plane, spot = lax.axis_index("plane"), spot_of()
    take_local(shared, plane, local_far, blocks, same_ref, lk_ref, lv_ref)
    take_global(plane, global_far, blocks, gk_ref, gv_ref)
    other = other_ref[...]

    def put(g, layer, acc):
        at = pl.multiple_of(g * HEAD, HEAD)
        out_ref[layer, :, pl.ds(at, HEAD)] = (acc[:, :HEAD] / acc[:, HEAD:]).astype(out_ref.dtype)

    def member(g, carry):
        low, high = carry
        q = jnp.concatenate([query_of(q_ref, 0, g), other], axis=1)
        put(g, 0, lacc_ref[g] + summed(q, lk_ref, lv_ref, rows, False))
        acc = gacc_ref[g] + summed(query_of(q_ref, 1, g), gk_ref, gv_ref, rows, False)
        put(g, 1, acc)
        totals = acc[:, HEAD:]
        low = jnp.minimum(low, jnp.min(totals, axis=0, keepdims=True))
        high = jnp.maximum(high, jnp.max(totals, axis=0, keepdims=True))
        return low, high

    ones = jnp.ones((1, HEAD), jnp.float32)
    low, high = lax.fori_loop(0, members, member, (ones, ones), unroll=n <= 4)
    safe = (jnp.min(low) > 2.0**-80) & (jnp.max(high) < 2.0**100)

    @pl.when(jnp.logical_not(safe))
    def _():
        take_global(plane, tuple(range(n)), blocks, allk_ref, allv_ref)

        def shifted(g, carry):
            q = query_of(q_ref, 1, g)
            peak, acc = None, None
            for first in range(0, n, 4):
                group = range(first, min(n, first + 4))
                used = slice(group[0] * rows, (group[-1] + 1) * rows)
                scores = lax.dot_general(q, allk_ref[used], NT, preferred_element_type=jnp.float32)
                scores = scores * (log2e * HEAD**-0.5)
                pieces = []
                for i in group:
                    piece = scores[:, (i - first) * rows : (i - first + 1) * rows]
                    allowed = causal(rows) if i == 0 else plane >= i
                    pieces.append(jnp.where(allowed, piece, masked_score))
                scores = jnp.concatenate(pieces, axis=1)
                top = jnp.max(scores, axis=1, keepdims=True)
                new_peak = top if peak is None else jnp.maximum(peak, top)
                if acc is not None:
                    acc = acc * jnp.exp2(peak - new_peak)
                peak = new_peak
                weights = jnp.exp2(scores - peak).astype(jnp.bfloat16)
                part = jnp.dot(weights, allv_ref[used], preferred_element_type=jnp.float32)
                acc = part if acc is None else acc + part
            put(g, 1, acc)
            return carry

        lax.fori_loop(0, members, shifted, 0)

    for s, o_ref in enumerate(o_refs):
        at = pl.ds(pl.multiple_of(lax.bitwise_xor(spot, s) * tokens, 16), tokens)
        o_ref[...] = out_ref[:, at]


def near(*arrays):
    if sum(x.size * x.dtype.itemsize for x in arrays) > near_bytes:
        return arrays
    return tuple(pltpu.with_memory_space_constraint(x, pltpu.VMEM) for x in arrays)


def exchange(x):
    return lax.all_to_all(x, IN_PLANE, split_axis=0, concat_axis=0, tiled=True)


def upward(x, by):
    size = lax.axis_size("plane")
    return lax.ppermute(x, "plane", [(i, i + by) for i in range(size - by)])


def unpack_body(parts, *refs):
    x_refs, o_refs, sems = refs[:parts], refs[parts:-1], refs[-1]
    width = x_refs[0].shape[2]
    spot = spot_of()
    copies = []
    for s, x_ref in enumerate(x_refs):
        at = pl.ds(pl.multiple_of(lax.bitwise_xor(spot, s) * width, HEAD), width)
        for layer, o_ref in enumerate(o_refs):
            copies.append(pltpu.make_async_copy(x_ref.at[layer], o_ref.at[:, at], sems.at[s, layer]))
    for copy in copies:
        copy.start()
    for copy in copies:
        copy.wait()


def unpack(pieces):
    parts = len(pieces)
    layers, tokens, width = pieces[0].shape
    shape = jax.ShapeDtypeStruct((tokens, parts * width), pieces[0].dtype)
    return pl.pallas_call(
        functools.partial(unpack_body, parts),
        out_shape=(shape,) * layers,
        in_specs=[pl.BlockSpec(memory_space=pltpu.VMEM)] * parts,
        out_specs=(pl.BlockSpec(memory_space=pl.ANY),) * layers,
        scratch_shapes=[pltpu.SemaphoreType.DMA((parts, layers))],
        cost_estimate=pl.CostEstimate(flops=0, bytes_accessed=4 * parts * pieces[0].size, transcendentals=0),
    )(*pieces)


def swapped(pieces):
    parts = len(pieces)
    came = [pieces[0]] * parts
    for s in partner_orders(parts):
        came[s] = lax.ppermute(pieces[s], IN_PLANE, [(i, i ^ s) for i in range(parts)])
    return came


def shards(query_local, key_local, value_local, labels, query_global, key_global, value_global):
    planes = lax.axis_size("plane")
    plane = lax.axis_index("plane")
    parts = lax.axis_size("row") * lax.axis_size("head")
    spot = lax.axis_index("row") * lax.axis_size("head") + lax.axis_index("head")
    tokens = query_local.shape[0]
    width = query_local.shape[1] // parts
    members = width // HEAD
    rows = parts * tokens
    dtype = query_local.dtype
    local_back = min(planes - 1, -(-(STRETCH - 1) // rows))

    packed = jax.ShapeDtypeStruct((parts, 4, tokens, HEAD), dtype)
    pack = vmem_call(pack_body, packed, 4, nbytes=16 * key_local.size)
    pack = pack(key_local, value_local, key_global, value_global)
    own = exchange(pack)
    blocks = [own]
    for d in range(1, planes):
        step = 1 if d < 3 else 3
        source = blocks[d - step]
        if d > local_back:
            source = source[:, source.shape[1] - 2 :]
        blocks.append(upward(source, step))

    bases = rope_tables(planes, rows)
    steps = rope_tables(rows, 1)
    turn = jnp.asarray(np.roll(np.eye(HEAD), HEAD // 2, axis=1), dtype)
    own_pos = plane * rows + spot * tokens + jnp.arange(tokens, dtype=jnp.int32)
    temper = 1.0 + temper_slope * jnp.log(((own_pos + 1) // temper_floor + 1).astype(jnp.float32))
    temper = jnp.broadcast_to(temper[:, None], (tokens, HEAD))
    label_row = labels[None, :]
    piece = jax.ShapeDtypeStruct((2, tokens, width), dtype)
    pack = vmem_call(
        pack_query_body, (piece,) * parts, 8, nbytes=8 * query_local.size, flops=2 * HEAD * query_local.size
    )
    queries = pack(query_local, query_global, *bases, *steps, turn, temper)
    queries = swapped(queries)

    global_near = tuple(d for d in range(planes) if d != 2) if planes <= 4 else (0, 1)
    global_far = tuple(d for d in range(planes) if d not in global_near)
    local_near = tuple(d for d in global_near if d <= local_back)
    local_far = tuple(d for d in global_far if d <= local_back)
    plan = (planes, parts, local_near, local_far, global_near, global_far)
    kept = near(*queries[1:], *blocks)
    queries, blocks = (queries[0], *kept[: parts - 1]), kept[parts - 1 :]
    shared = (*bases, *steps, turn)
    placed = jax.ShapeDtypeStruct((2, rows, width), dtype)
    sums = jax.ShapeDtypeStruct((members, rows, 2 * HEAD), jnp.float32)
    other = jax.ShapeDtypeStruct((rows, HEAD), dtype)
    same = jax.ShapeDtypeStruct((len(local_far), rows, HEAD), dtype)

    def cost(count):
        return dict(flops=6 * rows * rows * HEAD * members * count, exps=rows * rows * members * count)

    def scratch(count, columns):
        return pltpu.VMEM((count * rows, columns), dtype)

    def keys_and_values(local, others):
        both = scratch(len(local), 2 * HEAD)
        return [both, both, scratch(len(others), HEAD), scratch(len(others), 2 * HEAD)]

    early = vmem_call(
        functools.partial(early_body, plan),
        (placed, sums, sums, other, same),
        6 + len(global_near) + parts,
        nbytes=8 * rows * width,
        scratch=keys_and_values(local_near, global_near),
        limit=vmem_bytes,
        **cost(len(local_near) + len(global_near)),
    )(label_row, *shared, *(blocks[d] for d in global_near), *queries)
    early = near(*early)
    out = vmem_call(
        functools.partial(late_body, plan),
        (piece,) * parts,
        5 + planes + 5,
        nbytes=8 * rows * width,
        scratch=[pltpu.VMEM((2, rows, width), dtype)]
        + keys_and_values(local_far, global_far)
        + [scratch(planes, HEAD), scratch(planes, 2 * HEAD)],
        limit=vmem_bytes,
        **cost(len(local_far) + len(global_far)),
    )(*shared, *blocks, *early)
    return unpack(near(*swapped(out)))


def solution(mesh):
    ctx, head = mesh.shape["ctx"], mesh.shape["head"]

    def run(*args):
        key_heads = args[1].shape[1] // HEAD
        row = max(1, key_heads // head)
        grid = Mesh(mesh.devices.reshape(ctx // row, row, head), ("plane", "row", "head"))
        spread = P(("plane", "row", "head"), None)
        return jax.shard_map(
            shards,
            mesh=grid,
            in_specs=(spread, spread, spread, P(), spread, spread, spread),
            out_specs=(spread, spread),
            check_vma=False,
        )(*args)

    return run
```

```python
import functools

import jax
import jax.numpy as jnp
import numpy as np
from jax import lax
from jax.experimental import pallas as pl
from jax.experimental.pallas import tpu as pltpu
from jax.sharding import Mesh
from jax.sharding import PartitionSpec as P


HEAD = 128
STRETCH = 768

rope_base = 500000.0
norm_epsilon = 1e-06
temper_floor = 8192
temper_slope = 0.1
masked_score = -1e30
log2e = 1.4426950408889634
far = 30000.0
near_bytes = 6 << 20
vmem_bytes = 40 << 20

IN_PLANE = ("row", "head")


def rope_tables(count, step):
    half = HEAD // 2
    frequency = rope_base ** (-(np.arange(HEAD) % half) * 2.0 / HEAD)
    angles = (np.arange(count) * step)[:, None] * frequency[None, :]
    sign = np.where(np.arange(HEAD) < half, -1.0, 1.0)
    return jnp.asarray(np.cos(angles), jnp.float32), jnp.asarray(np.sin(angles) * sign, jnp.float32)


def turned(cos_base, sin_base, cos_row, sin_row):
    return cos_base * cos_row - sin_base * sin_row, sin_base * cos_row + cos_base * sin_row


def rotated_unit(x, turn, cosine, sine):
    swapped = jnp.dot(x, turn, preferred_element_type=jnp.float32)
    y = x.astype(jnp.float32) * cosine + swapped * sine
    return y * lax.rsqrt(jnp.mean(y * y, axis=-1, keepdims=True) + norm_epsilon)


def spot_of():
    return lax.axis_index("row") * lax.axis_size("head") + lax.axis_index("head")


def partner_orders(parts):
    return sorted(range(1, parts), key=lambda s: (s & 1, -s)) if parts > 1 else []


def vmem_call(body, out_shapes, n_in, flops=0, nbytes=0, exps=0, scratch=(), smem=0, limit=None):
    return pl.pallas_call(
        body,
        out_shape=out_shapes,
        in_specs=[pl.BlockSpec(memory_space=pltpu.SMEM)] * smem
        + [pl.BlockSpec(memory_space=pltpu.VMEM)] * n_in,
        out_specs=jax.tree.map(lambda _: pl.BlockSpec(memory_space=pltpu.VMEM), out_shapes),
        scratch_shapes=list(scratch),
        compiler_params=pltpu.CompilerParams(vmem_limit_bytes=limit),
        cost_estimate=pl.CostEstimate(flops=flops, bytes_accessed=nbytes, transcendentals=exps),
    )


def pack_body(kl_ref, vl_ref, kg_ref, vg_ref, o_ref):
    for d in range(o_ref.shape[0]):
        for a, ref in enumerate((kl_ref, vl_ref, kg_ref, vg_ref)):
            o_ref[d, a] = ref[:, d * HEAD : (d + 1) * HEAD]


def pack_query_body(ql_ref, qg_ref, cosb_ref, sinb_ref, cosr_ref, sinr_ref, turn_ref, temper_ref, *o_refs):
    tokens, width = ql_ref.shape[0], o_refs[0].shape[2]
    spot = spot_of()
    base, mine = pl.ds(lax.axis_index("plane"), 1), pl.ds(pl.multiple_of(spot * tokens, 16), tokens)
    cosine, sine = turned(cosb_ref[base], sinb_ref[base], cosr_ref[mine], sinr_ref[mine])
    turn = turn_ref[...]
    for s, o_ref in enumerate(o_refs):
        to = lax.bitwise_xor(spot, s)
        for g in range(width // HEAD):
            at = pl.ds(pl.multiple_of(to * width + g * HEAD, HEAD), HEAD)
            out = slice(g * HEAD, (g + 1) * HEAD)
            o_ref[0, :, out] = rotated_unit(ql_ref[:, at], turn, cosine, sine).astype(o_ref.dtype)
            o_ref[1, :, out] = (qg_ref[:, at].astype(jnp.float32) * temper_ref[...]).astype(o_ref.dtype)


def row_order(parts):
    return [*partner_orders(parts), 0]


def causal(distances, tokens, columns):
    spot = spot_of()
    row = lax.broadcasted_iota(jnp.int32, (tokens, columns), 0)
    token = jnp.concatenate([lax.bitwise_xor(spot, s) * tokens + row for s in distances], axis=0)
    return lax.broadcasted_iota(jnp.int32, token.shape, 1) <= token


def masked(weights, allowed):
    rows = allowed.shape[1]
    first = jnp.where(allowed, weights[:, :rows], 0.0)
    if weights.shape[1] == rows:
        return first
    return jnp.concatenate([first, weights[:, rows:]], axis=1)


NT = (((1,), (1,)), ((), ()))


def take_values(v_ref, i, values, valid):
    rows = values.shape[0]
    v_ref[i * rows : (i + 1) * rows, :HEAD] = values
    ones = jnp.broadcast_to(jnp.where(valid, 1.0, 0.0), (rows, HEAD))
    v_ref[i * rows : (i + 1) * rows, HEAD:] = ones.astype(v_ref.dtype)


def same_stretch(labels_ref, behind, rows):
    ids = labels_ref[:, pl.ds(pl.multiple_of(behind * rows, HEAD), rows)]
    return jnp.where(lax.broadcasted_iota(jnp.int32, (HEAD, rows), 0) == ids, 1.0, 0.0).T


def take_local(shared, plane, distances, blocks, same, k_ref, v_ref):
    cosb_ref, sinb_ref, cosr_ref, sinr_ref, turn_ref = shared
    turn = turn_ref[...]
    for i, d in enumerate(distances):
        rows = k_ref.shape[0] // len(distances)
        base = pl.ds(jnp.maximum(plane - d, 0), 1)
        cosine, sine = turned(cosb_ref[base], sinb_ref[base], cosr_ref[...], sinr_ref[...])
        at = slice(i * rows, (i + 1) * rows)
        keys = blocks[d][:, 0].reshape(rows, HEAD)
        k_ref[at, :HEAD] = rotated_unit(keys, turn, cosine, sine).astype(k_ref.dtype)
        k_ref[at, HEAD:] = same[i].astype(k_ref.dtype)
        take_values(v_ref, i, blocks[d][:, 1].reshape(rows, HEAD), plane >= d)


def take_global(plane, distances, blocks, k_ref, v_ref):
    for i, d in enumerate(distances):
        rows = k_ref.shape[0] // len(distances)
        last = blocks[d].shape[1] - 1
        k_ref[i * rows : (i + 1) * rows] = blocks[d][:, last - 1].reshape(rows, HEAD)
        take_values(v_ref, i, blocks[d][:, last].reshape(rows, HEAD), plane >= d)


def query_of(q_ref, layer, g):
    return q_ref[layer, :, pl.ds(pl.multiple_of(g * HEAD, HEAD), HEAD)]


def summed(q, k_ref, v_ref, rows, allowed):
    acc = None
    for at in range(0, k_ref.shape[0], 4 * rows):
        used = slice(at, min(k_ref.shape[0], at + 4 * rows))
        scores = lax.dot_general(q, k_ref[used], NT, preferred_element_type=jnp.float32)
        weights = jnp.exp2(scores * (log2e * HEAD**-0.5))
        if allowed is not None and at == 0:
            weights = masked(weights, allowed)
        part = jnp.dot(weights.astype(jnp.bfloat16), v_ref[used], preferred_element_type=jnp.float32)
        acc = part if acc is None else acc + part
    return acc


def early_body(plan, labels_ref, *refs):
    _, n_queries, local_near, local_far, global_near, _ = plan
    shared, refs = refs[:5], refs[5:]
    blocks = dict(zip(global_near, refs))
    queries, refs = refs[len(blocks) : len(blocks) + n_queries], refs[len(blocks) + n_queries :]
    q_ref, lacc_ref, gacc_ref, other_ref, same_ref, lk_ref, lv_ref, gk_ref, gv_ref = refs
    members, rows, _ = lacc_ref.shape
    tokens = rows // n_queries
    plane, spot = lax.axis_index("plane"), spot_of()
    order = row_order(n_queries)
    for i, s in enumerate(order):
        q_ref[:, i * tokens : (i + 1) * tokens] = queries[s][...]
    same = [same_stretch(labels_ref, jnp.maximum(plane - d, 0), rows) for d in local_near]
    for i, d in enumerate(local_far):
        same_ref[i] = same_stretch(labels_ref, jnp.maximum(plane - d, 0), rows).astype(same_ref.dtype)
    take_local(shared, plane, local_near, blocks, same, lk_ref, lv_ref)
    take_global(plane, global_near, blocks, gk_ref, gv_ref)
    for i, s in enumerate(order):
        at = pl.ds(pl.multiple_of(lax.bitwise_xor(spot, s) * tokens, 16), tokens)
        other_ref[i * tokens : (i + 1) * tokens] = ((lk_ref[at, HEAD:] - 1.0) * far).astype(other_ref.dtype)
    other = other_ref[...]
    allowed = causal(order, tokens, rows)

    def member(g, carry):
        q = jnp.concatenate([query_of(q_ref, 0, g), other], axis=1)
        lacc_ref[g] = summed(q, lk_ref, lv_ref, rows, allowed)
        gacc_ref[g] = summed(query_of(q_ref, 1, g), gk_ref, gv_ref, rows, allowed)
        return carry

    lax.fori_loop(0, members, member, 0, unroll=True)


def late_body(plan, first, count, *refs):
    n, n_queries, _, local_far, _, global_far = plan
    blocks, refs = refs[:n], refs[n:]
    q_ref, lacc_ref, gacc_ref, other_ref = refs[:4]
    plane = lax.axis_index("plane")
    if first == 0:
        same_ref, shared, refs = refs[4], refs[5:10], refs[10:]
        o_refs, ready, (allk_ref, allv_ref) = refs[:count], refs[count : count + 4], refs[count + 4 :]
        take_local(shared, plane, local_far, blocks, same_ref, *ready[:2])
        take_global(plane, global_far, blocks, *ready[2:])
    else:
        ready, o_refs, (allk_ref, allv_ref) = refs[4:8], refs[8 : 8 + count], refs[8 + count :]
    lk_ref, lv_ref, gk_ref, gv_ref = ready
    members, rows, _ = lacc_ref.shape
    tokens = rows // n_queries
    distances = row_order(n_queries)[first : first + count]
    mine = slice(first * tokens, (first + count) * tokens)
    other = other_ref[mine]

    def query_of(q_ref, layer, g):
        return q_ref[layer, mine, pl.ds(pl.multiple_of(g * HEAD, HEAD), HEAD)]

    def put(g, layer, acc):
        at = pl.ds(pl.multiple_of(g * HEAD, HEAD), HEAD)
        out = (acc[:, :HEAD] / acc[:, HEAD:]).astype(o_refs[0].dtype)
        for i, o_ref in enumerate(o_refs):
            o_ref[layer, :, at] = out[i * tokens : (i + 1) * tokens]

    def member(g, carry):
        low, high = carry
        q = jnp.concatenate([query_of(q_ref, 0, g), other], axis=1)
        put(g, 0, lacc_ref[g, mine] + summed(q, lk_ref, lv_ref, rows, None))
        acc = gacc_ref[g, mine] + summed(query_of(q_ref, 1, g), gk_ref, gv_ref, rows, None)
        put(g, 1, acc)
        totals = acc[:, HEAD:]
        low = jnp.minimum(low, jnp.min(totals, axis=0, keepdims=True))
        high = jnp.maximum(high, jnp.max(totals, axis=0, keepdims=True))
        return low, high

    ones = jnp.ones((1, HEAD), jnp.float32)
    low, high = lax.fori_loop(0, members, member, (ones, ones), unroll=n <= 4)
    safe = (jnp.min(low) > 2.0**-80) & (jnp.max(high) < 2.0**100)

    @pl.when(jnp.logical_not(safe))
    def _():
        take_global(plane, tuple(range(n)), blocks, allk_ref, allv_ref)

        def shifted(g, carry):
            q = query_of(q_ref, 1, g)
            peak, acc = None, None
            for first in range(0, n, 4):
                group = range(first, min(n, first + 4))
                used = slice(group[0] * rows, (group[-1] + 1) * rows)
                scores = lax.dot_general(q, allk_ref[used], NT, preferred_element_type=jnp.float32)
                scores = scores * (log2e * HEAD**-0.5)
                pieces = []
                for i in group:
                    piece = scores[:, (i - first) * rows : (i - first + 1) * rows]
                    allowed = causal(distances, tokens, rows) if i == 0 else plane >= i
                    pieces.append(jnp.where(allowed, piece, masked_score))
                scores = jnp.concatenate(pieces, axis=1)
                top = jnp.max(scores, axis=1, keepdims=True)
                new_peak = top if peak is None else jnp.maximum(peak, top)
                if acc is not None:
                    acc = acc * jnp.exp2(peak - new_peak)
                peak = new_peak
                weights = jnp.exp2(scores - peak).astype(jnp.bfloat16)
                part = jnp.dot(weights, allv_ref[used], preferred_element_type=jnp.float32)
                acc = part if acc is None else acc + part
            put(g, 1, acc)
            return carry

        lax.fori_loop(0, members, shifted, 0)


def near(*arrays):
    if sum(x.size * x.dtype.itemsize for x in arrays) > near_bytes:
        return arrays
    return tuple(pltpu.with_memory_space_constraint(x, pltpu.VMEM) for x in arrays)


def exchange(x):
    return lax.all_to_all(x, IN_PLANE, split_axis=0, concat_axis=0, tiled=True)


def upward(x, by):
    size = lax.axis_size("plane")
    return lax.ppermute(x, "plane", [(i, i + by) for i in range(size - by)])


def unpack_body(parts, *refs):
    x_refs, o_refs, sems = refs[:parts], refs[parts:-1], refs[-1]
    width = x_refs[0].shape[2]
    spot = spot_of()
    copies = []
    for s, x_ref in enumerate(x_refs):
        at = pl.ds(pl.multiple_of(lax.bitwise_xor(spot, s) * width, HEAD), width)
        for layer, o_ref in enumerate(o_refs):
            copies.append(pltpu.make_async_copy(x_ref.at[layer], o_ref.at[:, at], sems.at[s, layer]))
    for copy in copies:
        copy.start()
    for copy in copies:
        copy.wait()


def unpack(pieces):
    parts = len(pieces)
    layers, tokens, width = pieces[0].shape
    shape = jax.ShapeDtypeStruct((tokens, parts * width), pieces[0].dtype)
    return pl.pallas_call(
        functools.partial(unpack_body, parts),
        out_shape=(shape,) * layers,
        in_specs=[pl.BlockSpec(memory_space=pltpu.VMEM)] * parts,
        out_specs=(pl.BlockSpec(memory_space=pl.ANY),) * layers,
        scratch_shapes=[pltpu.SemaphoreType.DMA((parts, layers))],
        cost_estimate=pl.CostEstimate(flops=0, bytes_accessed=4 * parts * pieces[0].size, transcendentals=0),
    )(*pieces)


def swapped(pieces):
    parts = len(pieces)
    came = [pieces[0]] * parts
    for s in partner_orders(parts):
        came[s] = lax.ppermute(pieces[s], IN_PLANE, [(i, i ^ s) for i in range(parts)])
    return came


def shards(query_local, key_local, value_local, labels, query_global, key_global, value_global):
    planes = lax.axis_size("plane")
    plane = lax.axis_index("plane")
    parts = lax.axis_size("row") * lax.axis_size("head")
    spot = lax.axis_index("row") * lax.axis_size("head") + lax.axis_index("head")
    tokens = query_local.shape[0]
    width = query_local.shape[1] // parts
    members = width // HEAD
    rows = parts * tokens
    dtype = query_local.dtype
    local_back = min(planes - 1, -(-(STRETCH - 1) // rows))

    packed = jax.ShapeDtypeStruct((parts, 4, tokens, HEAD), dtype)
    pack = vmem_call(pack_body, packed, 4, nbytes=16 * key_local.size)
    pack = pack(key_local, value_local, key_global, value_global)
    own = exchange(pack)
    blocks = [own]
    for d in range(1, planes):
        step = 1 if d < 3 else 3
        source = blocks[d - step]
        if d > local_back:
            source = source[:, source.shape[1] - 2 :]
        blocks.append(upward(source, step))

    bases = rope_tables(planes, rows)
    steps = rope_tables(rows, 1)
    turn = jnp.asarray(np.roll(np.eye(HEAD), HEAD // 2, axis=1), dtype)
    own_pos = plane * rows + spot * tokens + jnp.arange(tokens, dtype=jnp.int32)
    temper = 1.0 + temper_slope * jnp.log(((own_pos + 1) // temper_floor + 1).astype(jnp.float32))
    temper = jnp.broadcast_to(temper[:, None], (tokens, HEAD))
    label_row = labels[None, :]
    piece = jax.ShapeDtypeStruct((2, tokens, width), dtype)
    pack = vmem_call(
        pack_query_body, (piece,) * parts, 8, nbytes=8 * query_local.size, flops=2 * HEAD * query_local.size
    )
    queries = pack(query_local, query_global, *bases, *steps, turn, temper)
    queries = swapped(queries)

    global_near = tuple(d for d in range(planes) if d != 2) if planes <= 4 else (0, 1)
    global_far = tuple(d for d in range(planes) if d not in global_near)
    local_near = tuple(d for d in global_near if d <= local_back)
    local_far = tuple(d for d in global_far if d <= local_back)
    plan = (planes, parts, local_near, local_far, global_near, global_far)
    kept = near(*queries[1:], *blocks)
    queries, blocks = (queries[0], *kept[: parts - 1]), kept[parts - 1 :]
    shared = (*bases, *steps, turn)
    placed = jax.ShapeDtypeStruct((2, rows, width), dtype)
    sums = jax.ShapeDtypeStruct((members, rows, 2 * HEAD), jnp.float32)
    other = jax.ShapeDtypeStruct((rows, HEAD), dtype)
    same = jax.ShapeDtypeStruct((len(local_far), rows, HEAD), dtype)

    def cost(count):
        return dict(flops=int(6 * rows * rows * HEAD * members * count), exps=int(rows * rows * members * count))

    def scratch(count, columns):
        return pltpu.VMEM((count * rows, columns), dtype)

    def keys_and_values(local, others):
        both = scratch(len(local), 2 * HEAD)
        return [both, both, scratch(len(others), HEAD), scratch(len(others), 2 * HEAD)]

    early = vmem_call(
        functools.partial(early_body, plan),
        (placed, sums, sums, other, same),
        6 + len(global_near) + parts,
        nbytes=8 * rows * width,
        scratch=keys_and_values(local_near, global_near),
        limit=vmem_bytes,
        **cost(len(local_near) + len(global_near)),
    )(label_row, *shared, *(blocks[d] for d in global_near), *queries)
    early = near(*early)
    placed, lacc, gacc, other, same = early
    half = parts // 2 + 1
    local_ready = jax.ShapeDtypeStruct((len(local_far) * rows, 2 * HEAD), dtype)
    key_ready = jax.ShapeDtypeStruct((len(global_far) * rows, HEAD), dtype)
    value_ready = jax.ShapeDtypeStruct((len(global_far) * rows, 2 * HEAD), dtype)
    late_options = dict(
        nbytes=4 * rows * width,
        scratch=[scratch(planes, HEAD), scratch(planes, 2 * HEAD)],
        limit=vmem_bytes,
        **cost((len(local_far) + len(global_far)) / 2),
    )
    first = vmem_call(
        functools.partial(late_body, plan, 0, half),
        (piece,) * half + (local_ready, local_ready, key_ready, value_ready),
        planes + 10,
        **late_options,
    )(*blocks, placed, lacc, gacc, other, same, *shared)
    first = near(*first)
    second = vmem_call(
        functools.partial(late_body, plan, half, parts - half),
        (piece,) * (parts - half),
        planes + 8,
        **late_options,
    )(*blocks, placed, lacc, gacc, other, *first[half:])
    out = dict(zip(row_order(parts), (*first[:half], *near(*second))))
    return unpack(swapped([out[s] for s in range(parts)]))


def solution(mesh):
    ctx, head = mesh.shape["ctx"], mesh.shape["head"]

    def run(*args):
        key_heads = args[1].shape[1] // HEAD
        row = max(1, key_heads // head)
        grid = Mesh(mesh.devices.reshape(ctx // row, row, head), ("plane", "row", "head"))
        spread = P(("plane", "row", "head"), None)
        return jax.shard_map(
            shards,
            mesh=grid,
            in_specs=(spread, spread, spread, P(), spread, spread, spread),
            out_specs=(spread, spread),
            check_vma=False,
        )(*args)

    return run
```
